128 devices in a mesh: hi: 64 (over y_lo, x, z, core), grp: 2 (over y_hi).
Axes of the slice: x: 4, y: 4 (y_hi: 2, y_lo: 2; y = y_hi * 2 + y_lo), z: 4, core: 2. Of those that a mesh axis runs over, the one named last changes fastest.
Arguments:
- rho: float32 [2, 8192, 8192], P(None, ('hi', 'grp')), may hold values from -6 to 9
- perm: int32 [2, 13], replicated, may hold values from 0 to 12, each once within a row
- superop: float32 [2, 2, 16, 16], replicated, may hold values from -0.3 to 1.1
Outputs:
- rho_out: float32 [2, 8192, 8192], P(None, ('hi', 'grp'))
- trace_mean: float32 [], replicated
The draws below stay inside these ranges and needn't reach their ends.
All inputs are finite; a program needn't handle non-finite values.
Results may differ from the reference program's by a relative error of at most 0.0001.
Values sent between devices are 32-bit elements; how exact they have to be, the bound alone decides.
No kernel may reach another device: no remote copies, remote signals or barrier semaphores. Data moves between devices by JAX's collectives and lax.ppermute only.
A program may use at most 256 MiB of HBM per device.

```python
import jax
import jax.numpy as jnp
from jax import lax

QUBITS = 13
ROWS = 8192
LAYERS = 2
PAIRS = 2


def draw_rho(key, part):
    noise = jnp.clip(jax.random.normal(key, (2, ROWS, ROWS), jnp.float32), -6.0, 6.0)
    ramp = 1.0 + 2.0 * jnp.arange(ROWS, dtype=jnp.float32) / ROWS
    diagonal = jnp.eye(ROWS, dtype=jnp.float32) * ramp[None, :]
    return noise.at[0].add(diagonal)


def draw_superop(key, part):
    noise = jnp.clip(0.06 * jax.random.normal(key, (LAYERS, 2, 16, 16), jnp.float32), -0.3, 0.3)
    return noise.at[:, 0].add(0.8 * jnp.eye(16, dtype=jnp.float32)[None])


def setup_inputs(seed: int = 0) -> dict:
    seeds = jax.random.split(jax.random.key(seed), 4)
    return {
        "rho": draw_rho(jax.random.fold_in(seeds[3], 71), 0),
        "perm": jax.vmap(lambda own: jax.random.permutation(own, QUBITS))(jax.random.split(seeds[1], LAYERS)).reshape((LAYERS, QUBITS)).astype(jnp.int32),
        "superop": draw_superop(jax.random.fold_in(seeds[3], 71), 0),
    }


def relabel_table(order, count):
    positions = jnp.arange(count, dtype=jnp.int32)
    result = jnp.zeros((count,), jnp.int32)
    for qubit in range(order.shape[0]):
        bit_value = jnp.bitwise_and(jnp.right_shift(positions, qubit), 1)
        result = result + bit_value * jnp.left_shift(jnp.int32(1), order[qubit].astype(jnp.int32))
    return result


def apply_channel(matrix, layer_super, pairs):
    real_part = layer_super[0]
    imag_part = layer_super[1]
    kernel = jnp.stack([jnp.stack([real_part, -imag_part], axis=1), jnp.stack([imag_part, real_part], axis=1)], axis=0)
    kernel = kernel.reshape(2, 4, 4, 2, 4, 4)
    row_count = matrix.shape[1]
    col_count = matrix.shape[2]
    for pair_idx in range(pairs):
        inner = 4 ** pair_idx
        shaped = matrix.reshape(2, row_count // (4 * inner), 4, inner, col_count // (4 * inner), 4, inner)
        shaped = jnp.einsum("ABCrst,rhsictj->AhBicCj", kernel, shaped, precision=lax.Precision.HIGHEST)
        matrix = shaped.reshape(2, row_count, col_count)
    return matrix


def reference(rho, perm, superop):
    matrix = rho
    for layer_idx in range(LAYERS):
        index_table = relabel_table(perm[layer_idx], ROWS)
        matrix = jnp.take(matrix, index_table, axis=1)
        matrix = jnp.take(matrix, index_table, axis=2)
        matrix = apply_channel(matrix, superop[layer_idx], PAIRS)
    trace_mean = jnp.trace(matrix[0]) / ROWS
    return matrix, trace_mean
```

```python
import jax
import jax.numpy as jnp
from jax import lax
from jax.experimental import pallas as pl
from jax.experimental.pallas import tpu as pltpu
from jax.sharding import PartitionSpec as P

ROWS = 8192
AX = ("hi", "grp")
RI = 13

W = 0
WINV = 16
U = 32
S0 = 48
A1 = 80
A2 = 112
C2 = 144
P1 = 176
SC = 208
RARE = 220
G = 224
OCCL = 320
OCCT = 328
OCCV = 336
OCCS = 340
TMP = 352
OCC = 384
USED = 400
SIZE = 432


def pick(cond, a, b):
    return jnp.where(cond, jnp.int32(a), jnp.int32(b))


def lane_swaps(T, base, targets, keep, slots, slot0):
    n = len(targets)
    for s in range(16):
        T[TMP + s] = jnp.int32(0)
        T[USED + s] = jnp.int32(0)
    for x in keep:
        T[TMP + x] = jnp.int32(1)
    for k, x in enumerate(targets):
        slot = jnp.int32(-1)
        for s in range(slots):
            slot = pick(T[OCCT + s] == x, s, slot)
        lane = jnp.int32(0)
        for p in range(7):
            lane = pick(T[TMP + T[OCCL + p]] == 0, p, lane)
        active = slot >= 0
        safe = jnp.maximum(slot, 0)
        old = T[OCCL + lane]
        T[OCCL + lane] = jnp.where(active, x, old)
        T[OCCT + safe] = jnp.where(active, old, T[OCCT + safe])
        T[USED + safe] = jnp.where(active, jnp.int32(1), T[USED + safe])
        T[base + 20 + k] = jnp.where(active, jnp.left_shift(jnp.int32(1), lane), 0)
        T[base + k] = slot
    for k in range(n):
        slot = T[base + k]
        free = jnp.int32(0)
        for s in range(slots):
            free = pick(T[USED + s] == 0, s, free)
        slot = jnp.where(slot >= 0, slot, free)
        T[USED + slot] = jnp.int32(1)
        stride = jnp.left_shift(jnp.int32(1), slot + slot0)
        T[base + k] = stride
        T[base + 10 + k] = stride
    for k in range(n, slots):
        free = jnp.int32(0)
        for s in range(slots):
            free = pick(T[USED + s] == 0, s, free)
        T[USED + free] = jnp.int32(1)
        stride = jnp.left_shift(jnp.int32(1), free + slot0)
        T[base + k] = stride
        T[base + 10 + k] = stride


def lane_of(T, x):
    lane = jnp.int32(0)
    for p in range(7):
        lane = pick(T[OCCL + p] == x, p, lane)
    return lane


def matrix_positions(T, base, pair):
    for p in range(7):
        T[TMP + p] = jnp.int32(0)
    for k, x in enumerate((jnp.int32(RI),) + pair):
        lane = lane_of(T, x)
        T[TMP + lane] = jnp.int32(1)
        T[base + k] = lane
    T[base + 3] = jnp.int32(7)
    T[base + 4] = jnp.int32(8)
    for k in range(4):
        free = jnp.int32(0)
        for p in range(7):
            free = pick(T[TMP + p] == 0, p, free)
        T[TMP + free] = jnp.int32(1)
        T[base + 5 + k] = free


def make_plan(perm, T):
    one = jnp.int32(1)
    for q in range(13):
        w = perm[0, perm[1, q]]
        T[W + q] = w
        T[WINV + w] = jnp.int32(q)
    for j in range(4):
        T[U + j] = perm[0, j]
    u = tuple(T[U + j] for j in range(4))
    w = tuple(T[W + q] for q in range(13))
    for p in range(8):
        T[OCCL + p] = jnp.int32(p)
    for s in range(7):
        T[OCCT + s] = jnp.int32(7 + s)
    head = (jnp.int32(RI),) + u
    lane_swaps(T, S0, head, head, 7, 0)
    for k in range(2):
        matrix_positions(T, G + 20 * k, (u[2 * k], u[2 * k + 1]))
    for b in range(16):
        T[TMP + b] = jnp.int32(0)
        T[USED + b] = jnp.int32(0)
    for j in range(4):
        T[TMP + u[j]] = one
    for s in range(10):
        T[OCC + s] = jnp.int32(3 + s)
    for i in range(3):
        mine_u = T[TMP + i]
        mine_ok = jnp.logical_and(mine_u == 0, T[WINV + i] < 6)
        best = jnp.int32(-1)
        spare = jnp.int32(-1)
        for b in range(3, 13):
            free = jnp.logical_and(T[TMP + b] == 0, T[USED + b] == 0)
            spare = pick(free, b, spare)
            best = pick(jnp.logical_and(free, T[WINV + b] < 6), b, best)
        other = jnp.where(mine_u == 0, -1, spare)
        bit = jnp.where(mine_ok, -1, jnp.where(best >= 0, best, other))
        active = bit >= 0
        safe = jnp.maximum(bit, 3)
        T[USED + safe] = jnp.where(active, one, T[USED + safe])
        T[P1 + i] = bit
        T[OCCS + i] = jnp.where(active, bit, jnp.int32(i))
        T[OCC + safe - 3] = jnp.where(active, jnp.int32(i), T[OCC + safe - 3])
        T[P1 + 20 + i] = pick(active, 1 << i, 0)
    T[P1 + 23] = jnp.int32(0)
    T[P1 + 24] = jnp.int32(0)
    for k in range(3):
        bit = T[P1 + k]
        free = jnp.int32(3)
        for b in range(3, 13):
            free = pick(T[USED + b] == 0, b, free)
        bit = jnp.where(bit >= 0, bit, free)
        T[USED + bit] = one
        T[P1 + k] = bit - 3
    for k in range(3, 10):
        free = jnp.int32(3)
        for b in range(3, 13):
            free = pick(T[USED + b] == 0, b, free)
        T[USED + free] = one
        T[P1 + k] = free - 3
    rare = jnp.int32(0)
    rare_amt = jnp.int32(0)
    rare_q = jnp.int32(6)
    for i in range(3):
        q = T[WINV + T[OCCS + i]]
        bad = q >= 6
        rare = pick(bad, 1, rare)
        rare_amt = pick(bad, 1 << i, rare_amt)
        rare_q = jnp.where(bad, q, rare_q)
    other = jnp.int32(0)
    kept = jnp.int32(0)
    rare_bit = jnp.int32(0)
    for s in range(10):
        occ = T[OCC + s]
        in_u = jnp.int32(-1)
        for j in range(4):
            in_u = pick(occ == u[j], 6 + j, in_u)
        place = jnp.where(in_u >= 0, in_u, other)
        other = jnp.where(in_u >= 0, other, other + 1)
        T[TMP + s] = place
        q = T[WINV + occ]
        is_kept = q < 6
        fits = kept < 3
        bit = jnp.where(is_kept, jnp.where(fits, kept, rare_q - 3), q - 3)
        slot = jnp.where(jnp.logical_and(is_kept, fits), kept, 3)
        T[OCCV + slot] = jnp.where(is_kept, occ, jnp.int32(0))
        rare_bit = jnp.where(jnp.logical_and(is_kept, jnp.logical_not(fits)), occ, rare_bit)
        kept = jnp.where(is_kept, kept + 1, kept)
        T[SC + place] = jnp.left_shift(one, bit)
    for i in range(3):
        q = T[WINV + T[OCCS + i]]
        T[OCCS + i] = jnp.where(q >= 6, rare_bit, T[OCCS + i])
    T[RARE] = rare
    T[RARE + 1] = jnp.left_shift(one, rare_q - 3)
    T[RARE + 2] = rare_amt
    for k in range(10):
        s = T[P1 + k]
        T[P1 + k] = jnp.left_shift(one, s)
        T[P1 + 10 + k] = jnp.left_shift(one, T[TMP + s])


def make_plan_2(T):
    one = jnp.int32(1)
    w = tuple(T[W + q] for q in range(13))
    head = w[:5]
    lane_swaps(T, A1, head, head + (jnp.int32(RI),), 7, 3)
    for k in range(3):
        T[A1 + 7 + k] = jnp.int32(1 << k)
        T[A1 + 17 + k] = jnp.int32(1 << k)
    matrix_positions(T, G + 40, (w[0], w[1]))
    for k in range(3):
        T[OCC + k] = 32 + T[OCCV + k]
    for k in range(7):
        T[OCC + 3 + k] = T[OCCT + k]
    for s in range(16):
        T[USED + s] = jnp.int32(0)
    for i in range(3):
        slot = jnp.int32(3)
        for s in range(3, 10):
            good = jnp.logical_and(T[USED + s] == 0, T[WINV + T[OCCT + s - 3]] >= 7)
            slot = pick(good, s, slot)
        T[USED + slot] = one
        T[A2 + i] = slot
        T[A2 + 20 + i] = jnp.int32(1 << i)
        col = T[OCC + slot]
        T[OCC + slot] = 32 + T[OCCS + i]
        T[OCCS + i] = col
    T[A2 + 23] = jnp.int32(0)
    T[A2 + 24] = jnp.int32(0)
    for k in range(3, 10):
        free = jnp.int32(3)
        for s in range(10):
            free = pick(T[USED + s] == 0, s, free)
        T[USED + free] = one
        T[A2 + k] = free
    other = jnp.int32(0)
    for s in range(10):
        occ = T[OCC + s]
        found = jnp.int32(-1)
        for j in range(4):
            found = pick(occ == 32 + w[j], 6 + j, found)
        place = jnp.where(found >= 0, found, other)
        other = jnp.where(found >= 0, other, other + 1)
        T[TMP + s] = place
    for s in range(10):
        T[USED + T[TMP + s]] = T[OCC + s]
    for k in range(10):
        s = T[A2 + k]
        T[A2 + k] = jnp.left_shift(one, s)
        T[A2 + 10 + k] = jnp.left_shift(one, T[TMP + s])
    for s in range(10):
        T[OCC + s] = T[USED + s]
    for i in range(3):
        T[OCC + 6 + i] = T[OCCS + i]
    last = jnp.int32(0)
    for p in range(7):
        x = T[OCCL + p]
        known = x == RI
        for q in range(5):
            known = jnp.logical_or(known, x == w[q])
        last = jnp.where(known, last, x)
    five = last == w[5]
    six = last == w[6]
    ri_lane = pick(five, 6, 5)
    last_lane = pick(five, 5, 6)
    g3 = G + 60
    pos = (jnp.int32(RI), w[2], w[3])
    for k, x in enumerate(pos):
        T[g3 + k] = lane_of(T, x)
    T[g3 + 3] = jnp.int32(7)
    T[g3 + 4] = jnp.int32(8)
    for k, x in enumerate((w[0], w[1], w[4], last)):
        T[g3 + 5 + k] = lane_of(T, x)
    for k, v in enumerate((ri_lane, 2, 3, 7, 8, 0, 1, 4, last_lane)):
        T[g3 + 9 + k] = jnp.int32(v)
    for s in range(10):
        T[USED + s] = jnp.int32(1 if 6 <= s <= 8 else 0)
    lane_swap = []
    for k in range(2):
        slot = jnp.int32(-1)
        for s in range(10):
            slot = pick(T[OCC + s] == w[5 + k], s, slot)
        active = slot >= 0
        safe = jnp.maximum(slot, 0)
        T[USED + safe] = jnp.where(active, one, T[USED + safe])
        T[C2 + 20 + 3 + k] = pick(active, 1 << (5 + k), 0)
        lane_x = jnp.where(ri_lane == 5 + k, jnp.int32(RI), last)
        T[OCC + safe] = jnp.where(active, lane_x, T[OCC + safe])
        lane_swap.append(slot)
    for k in range(2):
        free = jnp.int32(0)
        for s in range(10):
            free = pick(T[USED + s] == 0, s, free)
        slot = jnp.where(lane_swap[k] >= 0, lane_swap[k], free)
        T[USED + slot] = one
        T[C2 + 3 + k] = slot
    for i in range(3):
        T[C2 + i] = jnp.int32(6 + i)
        T[C2 + 20 + i] = jnp.int32(1 << i)
    for k in range(5, 10):
        free = jnp.int32(0)
        for s in range(10):
            free = pick(T[USED + s] == 0, s, free)
        T[USED + free] = one
        T[C2 + k] = free
    for k in range(10):
        s = T[C2 + k]
        occ = T[OCC + s]
        is_row = occ >= 32
        q = T[WINV + jnp.where(is_row, occ - 32, jnp.minimum(occ, 12))]
        bit = jnp.where(is_row, q + 3, q - 7)
        bit = jnp.where(occ == RI, 9, bit)
        T[C2 + k] = jnp.left_shift(one, s)
        T[C2 + 10 + k] = jnp.left_shift(one, bit)


def swap_pass(T, base, kinds, outer, load, store, table_dst=True):
    src = [T[base + k] for k in range(5 + outer)]
    dst = [T[base + 10 + k] for k in range(5 + outer)] if table_dst else src
    amounts = [T[base + 20 + k] for k in range(5)]
    lane = lax.broadcasted_iota(jnp.int32, (8, 128), 1)
    sub = lax.broadcasted_iota(jnp.int32, (8, 128), 0)
    keep_a = []
    keep_b = []
    for k, kind in enumerate(kinds):
        index = lane if kind == "l" else sub
        hit = jnp.bitwise_and(index, amounts[k])
        keep_a.append(hit == 0)
        keep_b.append(hit == amounts[k])

    def offsets(strides):
        offs = [jnp.int32(0)]
        for k in range(5):
            offs = offs + [o + strides[k] for o in offs]
        return offs

    src_offs = offsets(src)
    dst_offs = offsets(dst) if table_dst else src_offs

    def block(b, carry):
        src_base = jnp.int32(0)
        dst_base = jnp.int32(0)
        for k in range(outer):
            bit = jnp.bitwise_and(jnp.right_shift(b, k), 1)
            src_base = src_base + bit * src[5 + k]
            dst_base = dst_base + bit * dst[5 + k]
        if not table_dst:
            dst_base = src_base
        vs = [load(src_base + src_offs[m]) for m in range(32)]
        for k, kind in enumerate(kinds):
            if kind == "l":
                up, down, axis = amounts[k], jnp.bitwise_and(128 - amounts[k], 127), 1
            else:
                up, down, axis = 1 << k, 8 - (1 << k), 0
            for m in range(32):
                if not m >> k & 1:
                    n = m | 1 << k
                    a, b_ = vs[m], vs[n]
                    vs[m] = jnp.where(keep_a[k], a, pltpu.roll(b_, up, axis))
                    vs[n] = jnp.where(keep_b[k], b_, pltpu.roll(a, down, axis))
        for m in range(32):
            store(dst_base + dst_offs[m], vs[m])
        return carry

    lax.fori_loop(0, 1 << outer, block, 0)


def tile_rows(t):
    return pl.ds(pl.multiple_of(t * 8, 8), 8)


def build_matrix(T, base, out_base, sup, gh_ref, gl_ref):
    real, imag = sup[0], sup[1]
    top = jnp.concatenate([real, -imag], axis=1)
    bottom = jnp.concatenate([imag, real], axis=1)
    kern = jnp.concatenate([top, bottom], axis=0)
    index_i = lax.broadcasted_iota(jnp.int32, (512, 32), 0)
    index_o = lax.broadcasted_iota(jnp.int32, (32, 512), 1)

    def code(index, start, first, count):
        total = jnp.zeros_like(index)
        place = {0: 4, 1: 0, 2: 1, 3: 2, 4: 3}
        for k in range(first, first + count):
            bit = jnp.bitwise_and(jnp.right_shift(index, T[start + k]), 1)
            total = total + jnp.left_shift(bit, place[k] if first == 0 else k - first)
        return total

    one_i = (code(index_i, base, 0, 5) == lax.broadcasted_iota(jnp.int32, (512, 32), 1)).astype(jnp.bfloat16)
    one_o = (code(index_o, out_base, 0, 5) == lax.broadcasted_iota(jnp.int32, (32, 512), 0)).astype(jnp.bfloat16)
    rest_i = code(lax.broadcasted_iota(jnp.int32, (512, 128), 0), base, 5, 4)
    rest_o = code(lax.broadcasted_iota(jnp.int32, (8, 512), 1), out_base, 5, 4)
    same = jnp.concatenate([rest_i] * 4, axis=1) == jnp.concatenate([rest_o] * 64, axis=0)
    kh = kern.astype(jnp.bfloat16)
    kl = (kern - kh.astype(jnp.float32)).astype(jnp.bfloat16)
    for part, ref in ((kh, gh_ref), (kl, gl_ref)):
        left = lax.dot_general(one_i, part, (((1,), (1,)), ((), ())), preferred_element_type=jnp.float32)
        full = jnp.dot(left.astype(jnp.bfloat16), one_o, preferred_element_type=jnp.float32)
        ref[...] = jnp.where(same, full, 0.0).astype(jnp.bfloat16)


def mix(parts, gh, gl):
    x = jnp.concatenate(parts, axis=1)
    xh = x.astype(jnp.bfloat16)
    xl = (x - xh.astype(jnp.float32)).astype(jnp.bfloat16)
    y = jnp.dot(xl, gh, preferred_element_type=jnp.float32)
    y = y + jnp.dot(xh, gl, preferred_element_type=jnp.float32)
    return y + jnp.dot(xh, gh, preferred_element_type=jnp.float32)


def split_kernel(perm, rho, out, T):
    @pl.when(pl.program_id(0) == 0)
    def _():
        make_plan(perm, T)
        make_plan_2(T)

    def load(t):
        ri = jnp.right_shift(t, 6)
        ct = jnp.bitwise_and(t, 63)
        return rho[ri, :, pl.ds(pl.multiple_of(ct * 128, 128), 128)]

    def store(t, v):
        out[t] = v

    swap_pass(T, S0, "lllll", 2, load, store, table_dst=False)


def first_kernel(T, sup, x, out, buf, gh0, gl0, gh1, gl1):
    build_matrix(T, G, G, sup, gh0, gl0)
    build_matrix(T, G + 20, G + 20, sup, gh1, gl1)

    def load(t):
        return x[tile_rows(t), :]

    def store(t, v):
        buf[tile_rows(t), :] = v

    swap_pass(T, P1, "sss", 5, load, store)

    def pair0(g, carry):
        rows = [pl.ds(pl.multiple_of((g * 4 + j) * 512, 512), 512) for j in range(4)]
        y = mix([buf[r, :] for r in rows], gh0[...], gl0[...])
        for j in range(4):
            buf[rows[j], :] = y[:, j * 128 : (j + 1) * 128]
        return carry

    lax.fori_loop(0, 4, pair0, 0)
    strides = [T[SC + k] for k in range(10)]
    offs = [jnp.int32(0)]
    for k in range(6):
        offs = offs + [o + strides[k] for o in offs]

    def pair1(h, carry):
        rows = [pl.ds(pl.multiple_of((h + 4 * j) * 512, 512), 512) for j in range(4)]
        y = mix([buf[r, :] for r in rows], gh1[...], gl1[...])
        base = jnp.bitwise_and(h, 1) * strides[6] + jnp.right_shift(h, 1) * strides[7]
        for j in range(4):
            start = base + (strides[8] if j & 1 else 0) + (strides[9] if j & 2 else 0)
            for n in range(64):
                out[tile_rows(start + offs[n]), :] = y[n * 8 : n * 8 + 8, j * 128 : (j + 1) * 128]
        return carry

    lax.fori_loop(0, 4, pair1, 0)

    @pl.when(T[RARE] == 1)
    def _():
        stride = T[RARE + 1]
        amount = T[RARE + 2]
        sub = lax.broadcasted_iota(jnp.int32, (8, 128), 0)
        hit = jnp.bitwise_and(sub, amount)

        def pair(b, carry):
            low = jnp.bitwise_and(b, stride - 1)
            t = (b - low) * 2 + low
            a_rows, b_rows = tile_rows(t), tile_rows(t + stride)
            a, c = out[a_rows, :], out[b_rows, :]
            up = pltpu.roll(c, amount, 0)
            down = pltpu.roll(a, 8 - amount, 0)
            out[a_rows, :] = jnp.where(hit == 0, a, up)
            out[b_rows, :] = jnp.where(hit == amount, c, down)
            return carry

        lax.fori_loop(0, 512, pair, 0)


def second_kernel(T, pos, sup, x, out, trace, buf, buf2, gh0, gl0, gh1, gl1):
    build_matrix(T, G + 40, G + 40, sup, gh0, gl0)
    build_matrix(T, G + 60, G + 69, sup, gh1, gl1)

    def load_x(t):
        return x[tile_rows(t), :]

    def load_1(t):
        return buf[tile_rows(t), :]

    def store_1(t, v):
        buf[tile_rows(t), :] = v

    def load_2(t):
        return buf2[tile_rows(t), :]

    def store_2(t, v):
        buf2[tile_rows(t), :] = v

    swap_pass(T, A1, "lllll", 5, load_x, store_1)
    swap_pass(T, A2, "sss", 5, load_1, store_2)

    def pair0(g, carry):
        rows = [pl.ds(pl.multiple_of((g * 4 + j) * 512, 512), 512) for j in range(4)]
        y = mix([buf2[r, :] for r in rows], gh0[...], gl0[...])
        for j in range(4):
            buf[rows[j], :] = y[:, j * 128 : (j + 1) * 128]
        return carry

    def pair1(h, carry):
        rows = [pl.ds(pl.multiple_of((h + 4 * j) * 512, 512), 512) for j in range(4)]
        y = mix([buf[r, :] for r in rows], gh1[...], gl1[...])
        for j in range(4):
            buf2[rows[j], :] = y[:, j * 128 : (j + 1) * 128]
        return carry

    lax.fori_loop(0, 4, pair0, 0)
    lax.fori_loop(0, 4, pair1, 0)

    def store(t, v):
        ri = jnp.right_shift(t, 9)
        rt = jnp.bitwise_and(jnp.right_shift(t, 6), 7)
        ct = jnp.bitwise_and(t, 63)
        out[ri, tile_rows(rt), pl.ds(pl.multiple_of(ct * 128, 128), 128)] = v

    swap_pass(T, C2, "sssll", 5, load_2, store)
    device = pos[0]
    start = pl.multiple_of(jnp.right_shift(device, 1) * 128, 128)
    block = out[0, :, pl.ds(start, 128)]
    row = lax.broadcasted_iota(jnp.int32, (64, 128), 0) + jnp.bitwise_and(device, 1) * 64
    hit = row == lax.broadcasted_iota(jnp.int32, (64, 128), 1)
    trace[0, 0] = jnp.sum(jnp.where(hit, block, 0.0))


SMEM = pl.BlockSpec(memory_space=pltpu.SMEM)
VMEM = pl.BlockSpec(memory_space=pltpu.VMEM)
MATRICES = [pltpu.VMEM((512, 512), jnp.bfloat16)] * 4
LIMIT = 60 << 20


def exchange(blocks):
    return lax.all_to_all(blocks, AX, split_axis=0, concat_axis=0, tiled=True)


def per_device(rho, perm, superop):
    blocks, table = pl.pallas_call(
        split_kernel,
        grid=(8,),
        in_specs=[SMEM, pl.BlockSpec((2, 8, 8192), lambda i: (0, i, 0))],
        out_specs=[pl.BlockSpec((128, 8, 128), lambda i: (0, i, 0)), SMEM],
        out_shape=[
            jax.ShapeDtypeStruct((128, 64, 128), jnp.float32),
            jax.ShapeDtypeStruct((SIZE,), jnp.int32),
        ],
        name="split",
    )(perm, rho)
    blocks = exchange(blocks)
    blocks = pl.pallas_call(
        first_kernel,
        in_specs=[SMEM, VMEM, VMEM],
        out_specs=VMEM,
        out_shape=jax.ShapeDtypeStruct((8192, 128), jnp.float32),
        scratch_shapes=[pltpu.VMEM((8192, 128), jnp.float32)] + MATRICES,
        compiler_params=pltpu.CompilerParams(vmem_limit_bytes=LIMIT),
        name="first",
    )(table, superop[0], blocks.reshape(8192, 128))
    blocks = exchange(blocks.reshape(128, 64, 128))
    device = lax.axis_index(AX).astype(jnp.int32).reshape(1)
    rho_out, trace = pl.pallas_call(
        second_kernel,
        in_specs=[SMEM, SMEM, VMEM, VMEM],
        out_specs=[VMEM, SMEM],
        out_shape=[
            jax.ShapeDtypeStruct((2, 64, 8192), jnp.float32),
            jax.ShapeDtypeStruct((1, 1), jnp.float32),
        ],
        scratch_shapes=[pltpu.VMEM((8192, 128), jnp.float32)] * 2 + MATRICES,
        compiler_params=pltpu.CompilerParams(vmem_limit_bytes=LIMIT),
        name="second",
    )(table, device, superop[1], blocks.reshape(8192, 128))
    parts = exchange(jnp.broadcast_to(trace[0, 0], (128, 1, 128)))
    return rho_out, jnp.sum(parts[:, 0, 0]) / ROWS


def solution(mesh):
    spec = P(None, AX, None)
    return jax.shard_map(
        per_device, mesh=mesh, in_specs=(spec, P(), P()), out_specs=(spec, P()), check_vma=False
    )
```

```python
import jax
import jax.numpy as jnp
from jax import lax
from jax.experimental import pallas as pl
from jax.experimental.pallas import tpu as pltpu
from jax.sharding import PartitionSpec as P

ROWS = 8192
AX = ("hi", "grp")
RI = 13

W = 0
WINV = 16
U = 32
S0 = 48
A1 = 80
A2 = 112
C2 = 144
P1 = 176
SC = 208
RARE = 220
G = 224
OCCL = 320
OCCT = 328
OCCV = 336
OCCS = 340
TMP = 352
OCC = 384
USED = 400
SIZE = 432


def pick(cond, a, b):
    return jnp.where(cond, jnp.int32(a), jnp.int32(b))


def lane_swaps(T, base, targets, keep, slots, slot0):
    n = len(targets)
    for s in range(16):
        T[TMP + s] = jnp.int32(0)
        T[USED + s] = jnp.int32(0)
    for x in keep:
        T[TMP + x] = jnp.int32(1)
    for k, x in enumerate(targets):
        slot = jnp.int32(-1)
        for s in range(slots):
            slot = pick(T[OCCT + s] == x, s, slot)
        lane = jnp.int32(0)
        for p in range(7):
            lane = pick(T[TMP + T[OCCL + p]] == 0, p, lane)
        active = slot >= 0
        safe = jnp.maximum(slot, 0)
        old = T[OCCL + lane]
        T[OCCL + lane] = jnp.where(active, x, old)
        T[OCCT + safe] = jnp.where(active, old, T[OCCT + safe])
        T[USED + safe] = jnp.where(active, jnp.int32(1), T[USED + safe])
        T[base + 20 + k] = jnp.where(active, jnp.left_shift(jnp.int32(1), lane), 0)
        T[base + k] = slot
    for k in range(n):
        slot = T[base + k]
        free = jnp.int32(0)
        for s in range(slots):
            free = pick(T[USED + s] == 0, s, free)
        slot = jnp.where(slot >= 0, slot, free)
        T[USED + slot] = jnp.int32(1)
        stride = jnp.left_shift(jnp.int32(1), slot + slot0)
        T[base + k] = stride
        T[base + 10 + k] = stride
    for k in range(n, slots):
        free = jnp.int32(0)
        for s in range(slots):
            free = pick(T[USED + s] == 0, s, free)
        T[USED + free] = jnp.int32(1)
        stride = jnp.left_shift(jnp.int32(1), free + slot0)
        T[base + k] = stride
        T[base + 10 + k] = stride


def lane_of(T, x):
    lane = jnp.int32(0)
    for p in range(7):
        lane = pick(T[OCCL + p] == x, p, lane)
    return lane


def matrix_positions(T, base, pair):
    for p in range(7):
        T[TMP + p] = jnp.int32(0)
    for k, x in enumerate((jnp.int32(RI),) + pair):
        lane = lane_of(T, x)
        T[TMP + lane] = jnp.int32(1)
        T[base + k] = lane
    T[base + 3] = jnp.int32(7)
    T[base + 4] = jnp.int32(8)
    for k in range(4):
        free = jnp.int32(0)
        for p in range(7):
            free = pick(T[TMP + p] == 0, p, free)
        T[TMP + free] = jnp.int32(1)
        T[base + 5 + k] = free


def make_plan_0(perm, T):
    for q in range(13):
        w = perm[0, perm[1, q]]
        T[W + q] = w
        T[WINV + w] = jnp.int32(q)
    for j in range(4):
        T[U + j] = perm[0, j]
    u = tuple(T[U + j] for j in range(4))
    for p in range(8):
        T[OCCL + p] = jnp.int32(p)
    for s in range(7):
        T[OCCT + s] = jnp.int32(7 + s)
    head = (jnp.int32(RI),) + u
    lane_swaps(T, S0, head, head, 7, 0)


def make_plan_1(T):
    one = jnp.int32(1)
    u = tuple(T[U + j] for j in range(4))
    for k in range(2):
        matrix_positions(T, G + 20 * k, (u[2 * k], u[2 * k + 1]))
    for b in range(16):
        T[TMP + b] = jnp.int32(0)
        T[USED + b] = jnp.int32(0)
    for j in range(4):
        T[TMP + u[j]] = one
    for s in range(10):
        T[OCC + s] = jnp.int32(3 + s)
    for i in range(3):
        mine_u = T[TMP + i]
        mine_ok = jnp.logical_and(mine_u == 0, T[WINV + i] < 6)
        best = jnp.int32(-1)
        spare = jnp.int32(-1)
        for b in range(3, 13):
            free = jnp.logical_and(T[TMP + b] == 0, T[USED + b] == 0)
            spare = pick(free, b, spare)
            best = pick(jnp.logical_and(free, T[WINV + b] < 6), b, best)
        other = jnp.where(mine_u == 0, -1, spare)
        bit = jnp.where(mine_ok, -1, jnp.where(best >= 0, best, other))
        active = bit >= 0
        safe = jnp.maximum(bit, 3)
        T[USED + safe] = jnp.where(active, one, T[USED + safe])
        T[P1 + i] = bit
        T[OCCS + i] = jnp.where(active, bit, jnp.int32(i))
        T[OCC + safe - 3] = jnp.where(active, jnp.int32(i), T[OCC + safe - 3])
        T[P1 + 20 + i] = pick(active, 1 << i, 0)
    T[P1 + 23] = jnp.int32(0)
    T[P1 + 24] = jnp.int32(0)
    for k in range(3):
        bit = T[P1 + k]
        free = jnp.int32(3)
        for b in range(3, 13):
            free = pick(T[USED + b] == 0, b, free)
        bit = jnp.where(bit >= 0, bit, free)
        T[USED + bit] = one
        T[P1 + k] = bit - 3
    for k in range(3, 10):
        free = jnp.int32(3)
        for b in range(3, 13):
            free = pick(T[USED + b] == 0, b, free)
        T[USED + free] = one
        T[P1 + k] = free - 3
    rare = jnp.int32(0)
    rare_amt = jnp.int32(0)
    rare_q = jnp.int32(6)
    for i in range(3):
        q = T[WINV + T[OCCS + i]]
        bad = q >= 6
        rare = pick(bad, 1, rare)
        rare_amt = pick(bad, 1 << i, rare_amt)
        rare_q = jnp.where(bad, q, rare_q)
    other = jnp.int32(0)
    kept = jnp.int32(0)
    rare_bit = jnp.int32(0)
    for s in range(10):
        occ = T[OCC + s]
        in_u = jnp.int32(-1)
        for j in range(4):
            in_u = pick(occ == u[j], 6 + j, in_u)
        place = jnp.where(in_u >= 0, in_u, other)
        other = jnp.where(in_u >= 0, other, other + 1)
        T[TMP + s] = place
        q = T[WINV + occ]
        is_kept = q < 6
        fits = kept < 3
        bit = jnp.where(is_kept, jnp.where(fits, kept, rare_q - 3), q - 3)
        slot = jnp.where(jnp.logical_and(is_kept, fits), kept, 3)
        T[OCCV + slot] = jnp.where(is_kept, occ, jnp.int32(0))
        rare_bit = jnp.where(jnp.logical_and(is_kept, jnp.logical_not(fits)), occ, rare_bit)
        kept = jnp.where(is_kept, kept + 1, kept)
        T[SC + place] = jnp.left_shift(one, bit)
    for i in range(3):
        q = T[WINV + T[OCCS + i]]
        T[OCCS + i] = jnp.where(q >= 6, rare_bit, T[OCCS + i])
    T[RARE] = rare
    T[RARE + 1] = jnp.left_shift(one, rare_q - 3)
    T[RARE + 2] = rare_amt
    for k in range(10):
        s = T[P1 + k]
        T[P1 + k] = jnp.left_shift(one, s)
        T[P1 + 10 + k] = jnp.left_shift(one, T[TMP + s])


def make_plan_2(T):
    one = jnp.int32(1)
    w = tuple(T[W + q] for q in range(13))
    head = w[:5]
    lane_swaps(T, A1, head, head + (jnp.int32(RI),), 7, 3)
    for k in range(3):
        T[A1 + 7 + k] = jnp.int32(1 << k)
        T[A1 + 17 + k] = jnp.int32(1 << k)
    matrix_positions(T, G + 40, (w[0], w[1]))
    for k in range(3):
        T[OCC + k] = 32 + T[OCCV + k]
    for k in range(7):
        T[OCC + 3 + k] = T[OCCT + k]
    for s in range(16):
        T[USED + s] = jnp.int32(0)
    for i in range(3):
        slot = jnp.int32(3)
        for s in range(3, 10):
            good = jnp.logical_and(T[USED + s] == 0, T[WINV + T[OCCT + s - 3]] >= 7)
            slot = pick(good, s, slot)
        T[USED + slot] = one
        T[A2 + i] = slot
        T[A2 + 20 + i] = jnp.int32(1 << i)
        col = T[OCC + slot]
        T[OCC + slot] = 32 + T[OCCS + i]
        T[OCCS + i] = col
    T[A2 + 23] = jnp.int32(0)
    T[A2 + 24] = jnp.int32(0)
    for k in range(3, 10):
        free = jnp.int32(3)
        for s in range(10):
            free = pick(T[USED + s] == 0, s, free)
        T[USED + free] = one
        T[A2 + k] = free
    other = jnp.int32(0)
    for s in range(10):
        occ = T[OCC + s]
        found = jnp.int32(-1)
        for j in range(4):
            found = pick(occ == 32 + w[j], 6 + j, found)
        place = jnp.where(found >= 0, found, other)
        other = jnp.where(found >= 0, other, other + 1)
        T[TMP + s] = place
    for s in range(10):
        T[USED + T[TMP + s]] = T[OCC + s]
    for k in range(10):
        s = T[A2 + k]
        T[A2 + k] = jnp.left_shift(one, s)
        T[A2 + 10 + k] = jnp.left_shift(one, T[TMP + s])
    for s in range(10):
        T[OCC + s] = T[USED + s]
    for i in range(3):
        T[OCC + 6 + i] = T[OCCS + i]
    last = jnp.int32(0)
    for p in range(7):
        x = T[OCCL + p]
        known = x == RI
        for q in range(5):
            known = jnp.logical_or(known, x == w[q])
        last = jnp.where(known, last, x)
    five = last == w[5]
    six = last == w[6]
    ri_lane = pick(five, 6, 5)
    last_lane = pick(five, 5, 6)
    g3 = G + 60
    pos = (jnp.int32(RI), w[2], w[3])
    for k, x in enumerate(pos):
        T[g3 + k] = lane_of(T, x)
    T[g3 + 3] = jnp.int32(7)
    T[g3 + 4] = jnp.int32(8)
    for k, x in enumerate((w[0], w[1], w[4], last)):
        T[g3 + 5 + k] = lane_of(T, x)
    for k, v in enumerate((ri_lane, 2, 3, 7, 8, 0, 1, 4, last_lane)):
        T[g3 + 9 + k] = jnp.int32(v)
    for s in range(10):
        T[USED + s] = jnp.int32(1 if 6 <= s <= 8 else 0)
    lane_swap = []
    for k in range(2):
        slot = jnp.int32(-1)
        for s in range(10):
            slot = pick(T[OCC + s] == w[5 + k], s, slot)
        active = slot >= 0
        safe = jnp.maximum(slot, 0)
        T[USED + safe] = jnp.where(active, one, T[USED + safe])
        T[C2 + 20 + 3 + k] = pick(active, 1 << (5 + k), 0)
        lane_x = jnp.where(ri_lane == 5 + k, jnp.int32(RI), last)
        T[OCC + safe] = jnp.where(active, lane_x, T[OCC + safe])
        lane_swap.append(slot)
    for k in range(2):
        free = jnp.int32(0)
        for s in range(10):
            free = pick(T[USED + s] == 0, s, free)
        slot = jnp.where(lane_swap[k] >= 0, lane_swap[k], free)
        T[USED + slot] = one
        T[C2 + 3 + k] = slot
    for i in range(3):
        T[C2 + i] = jnp.int32(6 + i)
        T[C2 + 20 + i] = jnp.int32(1 << i)
    for k in range(5, 10):
        free = jnp.int32(0)
        for s in range(10):
            free = pick(T[USED + s] == 0, s, free)
        T[USED + free] = one
        T[C2 + k] = free
    for k in range(10):
        s = T[C2 + k]
        occ = T[OCC + s]
        is_row = occ >= 32
        q = T[WINV + jnp.where(is_row, occ - 32, jnp.minimum(occ, 12))]
        bit = jnp.where(is_row, q + 3, q - 7)
        bit = jnp.where(occ == RI, 9, bit)
        T[C2 + k] = jnp.left_shift(one, s)
        T[C2 + 10 + k] = jnp.left_shift(one, bit)


def swap_pass(T, base, kinds, outer, load, store, src=None):
    if src is None:
        src = [T[base + k] * 8 for k in range(5 + outer)]
    dst = [T[base + 10 + k] * 8 for k in range(5 + outer)]
    amounts = [T[base + 20 + k] for k in range(5)]
    lane = lax.broadcasted_iota(jnp.int32, (8, 128), 1)
    sub = lax.broadcasted_iota(jnp.int32, (8, 128), 0)
    keep_a = []
    keep_b = []
    partner = []
    for k, kind in enumerate(kinds):
        index = lane if kind == "l" else sub
        hit = jnp.bitwise_and(index, amounts[k])
        keep_a.append(hit == 0)
        keep_b.append(hit == amounts[k])
        partner.append(jnp.bitwise_xor(lane, amounts[k]))

    def sums(start, strides):
        out = [start]
        for stride in strides:
            out = out + [o + stride for o in out]
        return out

    src_low = sums(jnp.int32(0), src[:3])
    dst_low = sums(jnp.int32(0), dst[:3])

    def block(b, carry):
        src_base = jnp.int32(0)
        dst_base = jnp.int32(0)
        for k in range(outer):
            bit = jnp.bitwise_and(jnp.right_shift(b, k), 1)
            src_base = src_base + bit * src[5 + k]
            dst_base = dst_base + bit * dst[5 + k]
        vs = []
        for high in sums(src_base, src[3:5]):
            vs.extend(load(high + low, n) for n, low in enumerate(src_low))
        for k, kind in enumerate(kinds):
            for m in range(32):
                if not m >> k & 1:
                    n = m | 1 << k
                    x, y = vs[m], vs[n]
                    if kind == "l":
                        moved = jnp.where(keep_a[k], y, x)
                        moved = jnp.take_along_axis(moved, partner[k], axis=1, mode="promise_in_bounds")
                        vs[m] = jnp.where(keep_a[k], x, moved)
                        vs[n] = jnp.where(keep_b[k], y, moved)
                    else:
                        vs[m] = jnp.where(keep_a[k], x, pltpu.roll(y, 1 << k, 0))
                        vs[n] = jnp.where(keep_b[k], y, pltpu.roll(x, 8 - (1 << k), 0))
        m = 0
        for high in sums(dst_base, dst[3:5]):
            for low in dst_low:
                store(high + low, vs[m])
                m += 1
        return carry

    lax.fori_loop(0, 1 << outer, block, 0)


def tile_rows(row):
    return pl.ds(pl.multiple_of(row, 8), 8)


def build_matrix(T, base, out_base, sup, gh_ref, gl_ref):
    real, imag = sup[0], sup[1]
    top = jnp.concatenate([real, -imag], axis=1)
    bottom = jnp.concatenate([imag, real], axis=1)
    kern = jnp.concatenate([top, bottom], axis=0)
    index_i = lax.broadcasted_iota(jnp.int32, (512, 32), 0)
    index_o = lax.broadcasted_iota(jnp.int32, (32, 512), 1)

    def code(index, start, first, count):
        total = jnp.zeros_like(index)
        place = {0: 4, 1: 0, 2: 1, 3: 2, 4: 3}
        for k in range(first, first + count):
            bit = jnp.bitwise_and(jnp.right_shift(index, T[start + k]), 1)
            total = total + jnp.left_shift(bit, place[k] if first == 0 else k - first)
        return total

    one_i = (code(index_i, base, 0, 5) == lax.broadcasted_iota(jnp.int32, (512, 32), 1)).astype(jnp.bfloat16)
    one_o = (code(index_o, out_base, 0, 5) == lax.broadcasted_iota(jnp.int32, (32, 512), 0)).astype(jnp.bfloat16)
    rest_i = code(lax.broadcasted_iota(jnp.int32, (512, 128), 0), base, 5, 4)
    rest_o = code(lax.broadcasted_iota(jnp.int32, (8, 512), 1), out_base, 5, 4)
    same = jnp.concatenate([rest_i] * 4, axis=1) == jnp.concatenate([rest_o] * 64, axis=0)
    kh = kern.astype(jnp.bfloat16)
    kl = (kern - kh.astype(jnp.float32)).astype(jnp.bfloat16)
    for part, ref in ((kh, gh_ref), (kl, gl_ref)):
        left = lax.dot_general(one_i, part, (((1,), (1,)), ((), ())), preferred_element_type=jnp.float32)
        full = jnp.dot(left.astype(jnp.bfloat16), one_o, preferred_element_type=jnp.float32)
        ref[...] = jnp.where(same, full, 0.0).astype(jnp.bfloat16)


def mix(parts, gh, gl):
    x = jnp.concatenate(parts, axis=1)
    xh = x.astype(jnp.bfloat16)
    xl = (x - xh.astype(jnp.float32)).astype(jnp.bfloat16)
    y = jnp.dot(xl, gh, preferred_element_type=jnp.float32)
    y = y + jnp.dot(xh, gl, preferred_element_type=jnp.float32)
    return y + jnp.dot(xh, gh, preferred_element_type=jnp.float32)


def split_kernel(perm, rho, out, T):
    @pl.when(pl.program_id(0) == 0)
    def _():
        make_plan_0(perm, T)

    rows = out.reshape(1024, 128)

    def load(lane, n):
        return rho[n & 1, :, pl.ds(pl.multiple_of(lane, 128), 128)]

    def store(row, v):
        rows[tile_rows(row), :] = v

    src = [jnp.int32(0)] + [T[S0 + k] * 128 for k in range(1, 7)]
    swap_pass(T, S0, "lllll", 2, load, store, src)


def prepare_kernel(first_table, sup, T, matrices):
    def copy(k, carry):
        T[k] = first_table[k]
        return carry

    lax.fori_loop(0, TMP, copy, 0)
    make_plan_1(T)
    make_plan_2(T)
    for k, (base, out_base) in enumerate(((G, G), (G + 20, G + 20), (G + 40, G + 40), (G + 60, G + 69))):
        build_matrix(T, base, out_base, sup[k // 2], matrices.at[2 * k], matrices.at[2 * k + 1])


def reader(ref):
    return lambda row, n: ref[tile_rows(row), :]


def writer(ref):
    def store(row, v):
        ref[tile_rows(row), :] = v

    return store


def mix_pass(src, dst, matrices, step, store=None):
    def body(g, carry):
        first = g * 4 if step == 1 else g
        rows = [pl.ds(pl.multiple_of((first + step * j) * 512, 512), 512) for j in range(4)]
        y = mix([src[r, :] for r in rows], matrices[0], matrices[1])
        for j in range(4):
            piece = y[:, j * 128 : (j + 1) * 128]
            if store is None:
                dst[rows[j], :] = piece
            else:
                store(g, j, piece)
        return carry

    lax.fori_loop(0, 4, body, 0)


def first_kernel(T, matrices_hbm, x, out, buf, matrices, sem):
    fetch = pltpu.make_async_copy(matrices_hbm.at[pl.ds(0, 4)], matrices, sem)
    fetch.start()
    swap_pass(T, P1, "sss", 5, reader(x), writer(buf))
    fetch.wait()
    mix_pass(buf, buf, matrices.at[pl.ds(0, 2)], 1)
    strides = [T[SC + k] * 8 for k in range(10)]
    low = [jnp.int32(0)]
    for k in range(3):
        low = low + [o + strides[k] for o in low]

    def scatter(h, j, piece):
        start = jnp.bitwise_and(h, 1) * strides[6] + jnp.right_shift(h, 1) * strides[7]
        if j & 1:
            start = start + strides[8]
        if j & 2:
            start = start + strides[9]
        high = [start]
        for k in range(3, 6):
            high = high + [o + strides[k] for o in high]
        for n in range(64):
            out[tile_rows(high[n >> 3] + low[n & 7]), :] = piece[n * 8 : n * 8 + 8, :]

    mix_pass(buf, None, matrices.at[pl.ds(2, 2)], 4, scatter)

    @pl.when(T[RARE] == 1)
    def _():
        stride = T[RARE + 1]
        amount = T[RARE + 2]
        sub = lax.broadcasted_iota(jnp.int32, (8, 128), 0)
        hit = jnp.bitwise_and(sub, amount)

        def pair(b, carry):
            low = jnp.bitwise_and(b, stride - 1)
            t = (b - low) * 2 + low
            a_rows, b_rows = tile_rows(t * 8), tile_rows((t + stride) * 8)
            a, c = out[a_rows, :], out[b_rows, :]
            up = pltpu.roll(c, amount, 0)
            down = pltpu.roll(a, 8 - amount, 0)
            out[a_rows, :] = jnp.where(hit == 0, a, up)
            out[b_rows, :] = jnp.where(hit == amount, c, down)
            return carry

        lax.fori_loop(0, 512, pair, 0)


def second_kernel(T, pos, matrices_hbm, x, out, trace, buf, buf2, matrices, sem):
    fetch = pltpu.make_async_copy(matrices_hbm.at[pl.ds(4, 4)], matrices, sem)
    fetch.start()
    swap_pass(T, A1, "lllll", 5, reader(x), writer(buf))
    swap_pass(T, A2, "sss", 5, reader(buf), writer(buf2))
    fetch.wait()
    mix_pass(buf2, buf, matrices.at[pl.ds(0, 2)], 1)
    mix_pass(buf, buf2, matrices.at[pl.ds(2, 2)], 4)
    swap_pass(T, C2, "sssll", 5, reader(buf2), writer(out))
    device = pos[0]
    column = jnp.right_shift(device, 1)
    shift = jnp.bitwise_and(device, 1) * 64
    sub = lax.broadcasted_iota(jnp.int32, (8, 128), 0)
    lane = lax.broadcasted_iota(jnp.int32, (8, 128), 1)
    total = jnp.zeros((8, 128), jnp.float32)
    for t in range(8):
        tile = out[tile_rows((t * 64 + column) * 8), :]
        total = total + jnp.where(lane == sub + (t * 8 + shift), tile, 0.0)
    trace[0, 0] = jnp.sum(total)


SMEM = pl.BlockSpec(memory_space=pltpu.SMEM)
VMEM = pl.BlockSpec(memory_space=pltpu.VMEM)
HBM = pl.BlockSpec(memory_space=pl.ANY)
LIMIT = 60 << 20
BUFFER = pltpu.VMEM((8192, 128), jnp.float32)
MATRICES = pltpu.VMEM((4, 512, 512), jnp.bfloat16)


def exchange(blocks):
    return lax.all_to_all(blocks, AX, split_axis=0, concat_axis=0, tiled=True)


def per_device(rho, perm, superop):
    blocks, table = pl.pallas_call(
        split_kernel,
        grid=(8,),
        in_specs=[SMEM, pl.BlockSpec((2, 8, 8192), lambda i: (0, i, 0))],
        out_specs=[pl.BlockSpec((128, 8, 128), lambda i: (0, i, 0)), SMEM],
        out_shape=[
            jax.ShapeDtypeStruct((128, 64, 128), jnp.float32),
            jax.ShapeDtypeStruct((SIZE,), jnp.int32),
        ],
        name="split",
    )(perm, rho)
    table, matrices = pl.pallas_call(
        prepare_kernel,
        in_specs=[SMEM, VMEM],
        out_specs=[SMEM, VMEM],
        out_shape=[
            jax.ShapeDtypeStruct((SIZE,), jnp.int32),
            jax.ShapeDtypeStruct((8, 512, 512), jnp.bfloat16),
        ],
        compiler_params=pltpu.CompilerParams(vmem_limit_bytes=LIMIT),
        name="prepare",
    )(table, superop)
    blocks = exchange(blocks)
    blocks = pl.pallas_call(
        first_kernel,
        in_specs=[SMEM, HBM, VMEM],
        out_specs=VMEM,
        out_shape=jax.ShapeDtypeStruct((8192, 128), jnp.float32),
        scratch_shapes=[BUFFER, MATRICES, pltpu.SemaphoreType.DMA],
        compiler_params=pltpu.CompilerParams(vmem_limit_bytes=LIMIT),
        name="first",
    )(table, matrices, blocks.reshape(8192, 128))
    blocks = exchange(blocks.reshape(128, 64, 128))
    device = lax.axis_index(AX).astype(jnp.int32).reshape(1)
    tiles, trace = pl.pallas_call(
        second_kernel,
        in_specs=[SMEM, SMEM, HBM, VMEM],
        out_specs=[VMEM, SMEM],
        out_shape=[
            jax.ShapeDtypeStruct((8192, 128), jnp.float32),
            jax.ShapeDtypeStruct((1, 1), jnp.float32),
        ],
        scratch_shapes=[BUFFER, BUFFER, MATRICES, pltpu.SemaphoreType.DMA],
        compiler_params=pltpu.CompilerParams(vmem_limit_bytes=LIMIT),
        name="second",
    )(table, device, matrices, blocks.reshape(8192, 128))
    rho_out = tiles.reshape(2, 8, 64, 8, 128).transpose(0, 1, 3, 2, 4).reshape(2, 64, 8192)
    parts = exchange(jnp.broadcast_to(trace[0, 0], (128, 1, 128)))
    return rho_out, jnp.sum(parts[:, 0, 0]) / ROWS


def solution(mesh):
    spec = P(None, AX, None)
    return jax.shard_map(
        per_device, mesh=mesh, in_specs=(spec, P(), P()), out_specs=(spec, P()), check_vma=False
    )
```

```python
import jax
import jax.numpy as jnp
from jax import lax
from jax.experimental import pallas as pl
from jax.experimental.pallas import tpu as pltpu
from jax.sharding import PartitionSpec as P

ROWS = 8192
AX = ("hi", "grp")
RI = 13

W = 0
WINV = 16
U = 32
S0 = 48
A2 = 80
C2 = 112
P1 = 176
SC = 208
RARE = 220
G = 224
OCCL = 320
OCCT = 328
OCCR = 336
SUBC = 344
TMP = 352
OCC = 384
USED = 400
SIZE = 432


def pick(cond, a, b):
    return jnp.where(cond, jnp.int32(a), jnp.int32(b))


def lane_of(T, lanes, x):
    lane = jnp.int32(0)
    for p in range(7):
        lane = pick(T[lanes + p] == x, p, lane)
    return lane


def other_lanes(T, base, taken):
    for p in range(7):
        T[TMP + p] = jnp.int32(0)
    for lane in taken:
        T[TMP + lane] = jnp.int32(1)
    for k in range(4):
        free = jnp.int32(0)
        for p in range(7):
            free = pick(T[TMP + p] == 0, p, free)
        T[TMP + free] = jnp.int32(1)
        T[base + 5 + k] = free


def fill_slots(T, base, done, slots=10):
    for k in range(slots):
        free = jnp.int32(0)
        for s in range(slots):
            free = pick(T[USED + s] == 0, s, free)
        if k < done:
            free = jnp.where(T[base + k] >= 0, T[base + k], free)
        T[USED + free] = jnp.int32(1)
        T[base + k] = free


def set_strides(T, base, target):
    for k in range(10):
        s = T[base + k]
        T[base + k] = jnp.left_shift(jnp.int32(1), s)
        T[base + 10 + k] = jnp.left_shift(jnp.int32(1), T[target + s])


def make_plan_0(perm, T):
    one = jnp.int32(1)
    for q in range(13):
        w = perm[0, perm[1, q]]
        T[W + q] = w
        T[WINV + w] = jnp.int32(q)
    for b in range(16):
        T[TMP + b] = jnp.int32(0)
        T[USED + b] = jnp.int32(0)
    for q in range(4):
        T[TMP + T[W + q]] = jnp.int32(2)
    for j in range(4):
        T[U + j] = perm[0, j]
        T[TMP + perm[0, j]] = one
    for _ in range(2):
        x = jnp.int32(0)
        for b in range(12, -1, -1):
            x = pick(T[TMP + b] == 0, b, x)
        T[TMP + x] = one
    for s in range(10):
        T[OCC + s] = jnp.int32(3 + s)
    for i in range(3):
        best = jnp.int32(-1)
        for s in range(10):
            good = jnp.logical_and(T[TMP + 3 + s] == 1, T[USED + s] == 0)
            best = pick(good, s, best)
        slot = jnp.where(T[TMP + i] == 1, -1, best)
        active = slot >= 0
        safe = jnp.maximum(slot, 0)
        T[USED + safe] = jnp.where(active, one, T[USED + safe])
        T[OCCL + i] = jnp.where(active, slot + 3, jnp.int32(i))
        T[OCC + safe] = jnp.where(active, jnp.int32(i), T[OCC + safe])
        T[S0 + i] = slot
        T[S0 + 20 + i] = pick(active, 1 << i, 0)
    fill_slots(T, S0, 3)
    kept = jnp.int32(0)
    sent = jnp.int32(0)
    for s in range(10):
        occ = T[OCC + s]
        is_kept = T[TMP + occ] == 1
        T[USED + s] = jnp.where(is_kept, kept, sent + 3)
        T[jnp.where(is_kept, OCCL + 3 + kept, OCCT + sent)] = occ
        kept = jnp.where(is_kept, kept + 1, kept)
        sent = jnp.where(is_kept, sent, sent + 1)
    T[OCCL + 6] = jnp.int32(RI)
    set_strides(T, S0, USED)


def make_plan_1(T):
    one = jnp.int32(1)
    u = tuple(T[U + j] for j in range(4))
    for k in range(2):
        base = G + 20 * k
        lanes = [lane_of(T, OCCL, x) for x in (RI, u[2 * k], u[2 * k + 1])]
        other_lanes(T, base, lanes)
        for p in range(3):
            T[base + p] = lanes[p]
        T[base + 3] = jnp.int32(7)
        T[base + 4] = jnp.int32(8)
    for b in range(16):
        T[TMP + b] = jnp.int32(0)
        T[USED + b] = jnp.int32(0)
    for j in range(4):
        T[TMP + u[j]] = one
    for s in range(10):
        T[OCC + s] = jnp.int32(3 + s)
    for i in range(3):
        mine_u = T[TMP + i]
        mine_ok = jnp.logical_and(mine_u == 0, T[WINV + i] < 6)
        best = jnp.int32(-1)
        spare = jnp.int32(-1)
        for b in range(3, 13):
            free = jnp.logical_and(T[TMP + b] == 0, T[USED + b - 3] == 0)
            spare = pick(free, b, spare)
            best = pick(jnp.logical_and(free, T[WINV + b] < 6), b, best)
        other = jnp.where(mine_u == 0, -1, spare)
        bit = jnp.where(mine_ok, -1, jnp.where(best >= 0, best, other))
        active = bit >= 0
        safe = jnp.maximum(bit, 3)
        T[USED + safe - 3] = jnp.where(active, one, T[USED + safe - 3])
        T[P1 + i] = jnp.where(active, bit - 3, -1)
        T[OCCR + i] = jnp.where(active, bit, jnp.int32(i))
        T[OCC + safe - 3] = jnp.where(active, jnp.int32(i), T[OCC + safe - 3])
        T[P1 + 20 + i] = pick(active, 1 << i, 0)
    fill_slots(T, P1, 3)
    rare = jnp.int32(0)
    rare_amt = jnp.int32(0)
    rare_q = jnp.int32(6)
    for i in range(3):
        q = T[WINV + T[OCCR + i]]
        bad = q >= 6
        rare = pick(bad, 1, rare)
        rare_amt = pick(bad, 1 << i, rare_amt)
        rare_q = jnp.where(bad, q, rare_q)
    other = jnp.int32(0)
    kept = jnp.int32(0)
    rare_bit = jnp.int32(0)
    for s in range(10):
        occ = T[OCC + s]
        in_u = jnp.int32(-1)
        for j in range(4):
            in_u = pick(occ == u[j], 6 + j, in_u)
        place = jnp.where(in_u >= 0, in_u, other)
        other = jnp.where(in_u >= 0, other, other + 1)
        T[TMP + s] = place
        q = T[WINV + occ]
        is_kept = q < 6
        fits = kept < 3
        bit = jnp.where(is_kept, jnp.where(fits, kept, rare_q - 3), q - 3)
        slot = jnp.where(jnp.logical_and(is_kept, fits), kept, 3)
        T[OCCR + 3 + slot] = jnp.where(is_kept, occ, jnp.int32(RI))
        rare_bit = jnp.where(jnp.logical_and(is_kept, jnp.logical_not(fits)), occ, rare_bit)
        kept = jnp.where(is_kept, kept + 1, kept)
        T[SC + place] = jnp.left_shift(one, bit)
    for i in range(3):
        q = T[WINV + T[OCCR + i]]
        T[OCCR + i] = jnp.where(q >= 6, rare_bit, T[OCCR + i])
    T[OCCR + 6] = jnp.int32(RI)
    T[RARE] = rare
    T[RARE + 1] = jnp.left_shift(one, rare_q - 3)
    T[RARE + 2] = rare_amt
    set_strides(T, P1, TMP)


def make_plan_2(T):
    one = jnp.int32(1)
    w = tuple(T[W + q] for q in range(13))
    for k in range(3):
        T[SUBC + k] = T[OCCL + k]
        T[OCC + k] = T[OCCL + 3 + k]
    for k in range(7):
        T[OCC + 3 + k] = T[OCCT + k]
    for s in range(16):
        T[USED + s] = jnp.int32(0)
    for i in range(3):
        mine = T[SUBC + i]
        best = jnp.int32(-1)
        for s in range(10):
            good = jnp.logical_and(T[WINV + T[OCC + s]] >= 4, T[USED + s] == 0)
            best = pick(good, s, best)
        slot = jnp.where(T[WINV + mine] >= 4, -1, best)
        active = slot >= 0
        safe = jnp.maximum(slot, 0)
        T[USED + safe] = jnp.where(active, one, T[USED + safe])
        new = T[OCC + safe]
        T[SUBC + i] = jnp.where(active, new, mine)
        T[OCC + safe] = jnp.where(active, mine, new)
        T[A2 + i] = slot
        T[A2 + 20 + i] = pick(active, 1 << i, 0)
    fill_slots(T, A2, 3)
    other = jnp.int32(0)
    for s in range(10):
        q = T[WINV + T[OCC + s]]
        T[TMP + s] = jnp.where(q < 4, q + 6, other)
        other = jnp.where(q < 4, other, other + 1)
    set_strides(T, A2, TMP)
    for s in range(10):
        T[USED + T[TMP + s]] = T[OCC + s]
    for s in range(10):
        T[OCC + s] = T[USED + s]
    rows = [lane_of(T, OCCR, w[q]) for q in range(6)]
    ri = lane_of(T, OCCR, RI)
    other_lanes(T, G + 40, (ri, rows[0], rows[1]))
    for k, v in enumerate((ri, 7, 8, rows[0], rows[1])):
        T[G + 40 + k] = jnp.int32(v)
    for k, v in enumerate((ri, 7, 8, rows[2], rows[3], rows[0], rows[1], rows[4], rows[5])):
        T[G + 60 + k] = jnp.int32(v)
    for k, v in enumerate((6, 7, 8, 2, 3, 0, 1, 4, 5)):
        T[G + 69 + k] = jnp.int32(v)
    for i in range(3):
        T[OCC + 6 + i] = T[SUBC + i]
    for s in range(10):
        T[USED + s] = jnp.int32(0)
        q = T[WINV + T[OCC + s]]
        T[TMP + s] = q - 7
    for k in range(4):
        slot = jnp.int32(0)
        for s in range(10):
            slot = pick(T[OCC + s] == w[3 + k], s, slot)
        T[USED + slot] = one
        T[C2 + k] = slot
        T[TMP + slot] = jnp.int32(6 + k)
    fill_slots(T, C2, 4)
    set_strides(T, C2, TMP)


def sums(start, strides):
    out = [start]
    for stride in strides:
        out = out + [o + stride for o in out]
    return out


def block_loop(src, dst, load, store, work):
    src_low = sums(jnp.int32(0), src[:3])
    dst_low = sums(jnp.int32(0), dst[:3])

    def block(b, carry):
        src_base = jnp.int32(0)
        dst_base = jnp.int32(0)
        for k in range(5):
            bit = jnp.bitwise_and(jnp.right_shift(b, k), 1)
            src_base = src_base + bit * src[5 + k]
            dst_base = dst_base + bit * dst[5 + k]
        vs = []
        for high in sums(src_base, src[3:5]):
            vs.extend(load[tile_rows(high + low), :] for low in src_low)
        vs = work(vs)
        m = 0
        for high in sums(dst_base, dst[3:5]):
            for low in dst_low:
                store[tile_rows(high + low), :] = vs[m]
                m += 1
        return carry

    lax.fori_loop(0, 32, block, 0)


def table_strides(T, base):
    return [T[base + k] * 8 for k in range(10)], [T[base + 10 + k] * 8 for k in range(10)]


def sublane_swaps(src, dst, load, store, amounts):
    sub = lax.broadcasted_iota(jnp.int32, (8, 128), 0)
    hits = [jnp.bitwise_and(sub, amount) for amount in amounts]
    keep_x = [hit == 0 for hit in hits]
    keep_y = [hit == amount for hit, amount in zip(hits, amounts)]

    def work(vs):
        for k in range(3):
            for m in range(32):
                if not m >> k & 1:
                    n = m | 1 << k
                    x, y = vs[m], vs[n]
                    vs[m] = jnp.where(keep_x[k], x, pltpu.roll(y, 1 << k, 0))
                    vs[n] = jnp.where(keep_y[k], y, pltpu.roll(x, 8 - (1 << k), 0))
        return vs

    block_loop(src, dst, load, store, work)


def table_swaps(T, base, load, store):
    src, dst = table_strides(T, base)
    sublane_swaps(src, dst, load, store, [T[base + 20 + k] for k in range(3)])


def transposes(T, base, load, store):
    src, dst = table_strides(T, base)

    def work(vs):
        out = []
        for half in range(2):
            y = jnp.concatenate(vs[16 * half : 16 * half + 16], axis=0).T
            out.extend(y[8 * m : 8 * m + 8, :] for m in range(16))
        return out

    block_loop(src, dst, load, store, work)


def turn(src, dst):
    low = lax.broadcasted_iota(jnp.int32, (64, 128), 1) < 64

    def body(d, carry):
        rows = [pl.ds(pl.multiple_of((d + k) * 64, 64), 64) for k in (0, 64)]
        y = jnp.concatenate([src[r, :] for r in rows], axis=0).T
        p, q = y[:64, :], y[64:, :]
        moved = pltpu.roll(jnp.where(low, q, p), 64, 1)
        dst[rows[0], :] = jnp.where(low, p, moved)
        dst[rows[1], :] = jnp.where(low, moved, q)
        return carry

    lax.fori_loop(0, 64, body, 0, unroll=4)


def tile_rows(row):
    return pl.ds(pl.multiple_of(row, 8), 8)


def build_matrix(T, base, out_base, sup, gh_ref, gl_ref):
    real, imag = sup[0], sup[1]
    top = jnp.concatenate([real, -imag], axis=1)
    bottom = jnp.concatenate([imag, real], axis=1)
    kern = jnp.concatenate([top, bottom], axis=0)
    index_i = lax.broadcasted_iota(jnp.int32, (512, 32), 0)
    index_o = lax.broadcasted_iota(jnp.int32, (32, 512), 1)

    def code(index, start, first, count):
        total = jnp.zeros_like(index)
        place = {0: 4, 1: 0, 2: 1, 3: 2, 4: 3}
        for k in range(first, first + count):
            bit = jnp.bitwise_and(jnp.right_shift(index, T[start + k]), 1)
            total = total + jnp.left_shift(bit, place[k] if first == 0 else k - first)
        return total

    one_i = (code(index_i, base, 0, 5) == lax.broadcasted_iota(jnp.int32, (512, 32), 1)).astype(jnp.bfloat16)
    one_o = (code(index_o, out_base, 0, 5) == lax.broadcasted_iota(jnp.int32, (32, 512), 0)).astype(jnp.bfloat16)
    rest_i = code(lax.broadcasted_iota(jnp.int32, (512, 128), 0), base, 5, 4)
    rest_o = code(lax.broadcasted_iota(jnp.int32, (8, 512), 1), out_base, 5, 4)
    same = jnp.concatenate([rest_i] * 4, axis=1) == jnp.concatenate([rest_o] * 64, axis=0)
    kh = kern.astype(jnp.bfloat16)
    kl = (kern - kh.astype(jnp.float32)).astype(jnp.bfloat16)
    for part, ref in ((kh, gh_ref), (kl, gl_ref)):
        left = lax.dot_general(one_i, part, (((1,), (1,)), ((), ())), preferred_element_type=jnp.float32)
        full = jnp.dot(left.astype(jnp.bfloat16), one_o, preferred_element_type=jnp.float32)
        ref[...] = jnp.where(same, full, 0.0).astype(jnp.bfloat16)


def mix(parts, gh, gl):
    x = jnp.concatenate(parts, axis=1)
    xh = x.astype(jnp.bfloat16)
    xl = (x - xh.astype(jnp.float32)).astype(jnp.bfloat16)
    y = jnp.dot(xl, gh, preferred_element_type=jnp.float32)
    y = y + jnp.dot(xh, gl, preferred_element_type=jnp.float32)
    return y + jnp.dot(xh, gh, preferred_element_type=jnp.float32)


def split_kernel(perm, rho, out, T, buf):
    step = pl.program_id(0)

    @pl.when(step == 0)
    def _():
        make_plan_0(perm, T)

    for c in range(8):
        lanes = slice(c * 128, c * 128 + 128)
        x = jnp.concatenate([rho[0, :, lanes], rho[1, :, lanes]], axis=0)
        buf[pl.ds(pl.multiple_of(step * 1024 + c * 128, 128), 128), :] = x.T

    @pl.when(step == 7)
    def _():
        table_swaps(T, S0, buf, out)


def prepare_kernel(first_table, sup, T, matrices):
    def copy(k, carry):
        T[k] = first_table[k]
        return carry

    lax.fori_loop(0, TMP, copy, 0)
    make_plan_1(T)
    make_plan_2(T)
    for k, (base, out_base) in enumerate(((G, G), (G + 20, G + 20), (G + 40, G + 40), (G + 60, G + 69))):
        build_matrix(T, base, out_base, sup[k // 2], matrices.at[2 * k], matrices.at[2 * k + 1])


def mix_pass(src, dst, matrices, step, store=None):
    def body(g, carry):
        first = g * 4 if step == 1 else g
        rows = [pl.ds(pl.multiple_of((first + step * j) * 512, 512), 512) for j in range(4)]
        y = mix([src[r, :] for r in rows], matrices[0], matrices[1])
        for j in range(4):
            piece = y[:, j * 128 : (j + 1) * 128]
            if store is None:
                dst[rows[j], :] = piece
            else:
                store(g, j, piece)
        return carry

    lax.fori_loop(0, 4, body, 0)


def first_kernel(T, matrices_hbm, x, out, buf, buf2, matrices, sem):
    fetch = pltpu.make_async_copy(matrices_hbm.at[pl.ds(0, 4)], matrices, sem)
    fetch.start()
    turn(x, buf)
    table_swaps(T, P1, buf, buf2)
    fetch.wait()
    mix_pass(buf2, buf2, matrices.at[pl.ds(0, 2)], 1)
    strides = [T[SC + k] * 8 for k in range(10)]
    low = [jnp.int32(0)]
    for k in range(3):
        low = low + [o + strides[k] for o in low]

    def scatter(h, j, piece):
        start = jnp.bitwise_and(h, 1) * strides[6] + jnp.right_shift(h, 1) * strides[7]
        if j & 1:
            start = start + strides[8]
        if j & 2:
            start = start + strides[9]
        high = [start]
        for k in range(3, 6):
            high = high + [o + strides[k] for o in high]
        for n in range(64):
            out[tile_rows(high[n >> 3] + low[n & 7]), :] = piece[n * 8 : n * 8 + 8, :]

    mix_pass(buf2, None, matrices.at[pl.ds(2, 2)], 4, scatter)

    @pl.when(T[RARE] == 1)
    def _():
        stride = T[RARE + 1]
        amount = T[RARE + 2]
        sub = lax.broadcasted_iota(jnp.int32, (8, 128), 0)
        hit = jnp.bitwise_and(sub, amount)

        def pair(b, carry):
            low = jnp.bitwise_and(b, stride - 1)
            t = (b - low) * 2 + low
            a_rows, b_rows = tile_rows(t * 8), tile_rows((t + stride) * 8)
            a, c = out[a_rows, :], out[b_rows, :]
            up = pltpu.roll(c, amount, 0)
            down = pltpu.roll(a, 8 - amount, 0)
            out[a_rows, :] = jnp.where(hit == 0, a, up)
            out[b_rows, :] = jnp.where(hit == amount, c, down)
            return carry

        lax.fori_loop(0, 512, pair, 0)


def second_kernel(T, pos, matrices_hbm, x, out, trace, buf, buf2, matrices, sem):
    fetch = pltpu.make_async_copy(matrices_hbm.at[pl.ds(4, 4)], matrices, sem)
    fetch.start()
    turn(x, buf)
    table_swaps(T, A2, buf, buf2)
    fetch.wait()
    mix_pass(buf2, buf, matrices.at[pl.ds(0, 2)], 1)
    mix_pass(buf, buf2, matrices.at[pl.ds(2, 2)], 4)
    slots = [8 << k for k in (6, 7, 8, 0, 1, 2, 3, 4, 5, 9)]
    sublane_swaps(slots, slots, buf2, buf, (1, 2, 4))
    transposes(T, C2, buf, out)
    device = pos[0]
    column = jnp.right_shift(device, 1)
    shift = jnp.bitwise_and(device, 1) * 64
    sub = lax.broadcasted_iota(jnp.int32, (8, 128), 0)
    lane = lax.broadcasted_iota(jnp.int32, (8, 128), 1)
    total = jnp.zeros((8, 128), jnp.float32)
    for t in range(8):
        tile = out[tile_rows((t * 64 + column) * 8), :]
        total = total + jnp.where(lane == sub + (t * 8 + shift), tile, 0.0)
    trace[0, 0] = jnp.sum(total)


SMEM = pl.BlockSpec(memory_space=pltpu.SMEM)
VMEM = pl.BlockSpec(memory_space=pltpu.VMEM)
HBM = pl.BlockSpec(memory_space=pl.ANY)
LIMIT = 60 << 20
BUFFER = pltpu.VMEM((8192, 128), jnp.float32)
MATRICES = pltpu.VMEM((4, 512, 512), jnp.bfloat16)


def exchange(blocks):
    return lax.all_to_all(blocks, AX, split_axis=0, concat_axis=0, tiled=True)


def per_device(rho, perm, superop):
    blocks, table = pl.pallas_call(
        split_kernel,
        grid=(8,),
        in_specs=[SMEM, pl.BlockSpec((2, 64, 1024), lambda i: (0, 0, i))],
        out_specs=[pl.BlockSpec((8192, 128), lambda i: (0, 0)), SMEM],
        scratch_shapes=[BUFFER],
        out_shape=[
            jax.ShapeDtypeStruct((8192, 128), jnp.float32),
            jax.ShapeDtypeStruct((SIZE,), jnp.int32),
        ],
        compiler_params=pltpu.CompilerParams(vmem_limit_bytes=LIMIT),
        name="split",
    )(perm, rho)
    table, matrices = pl.pallas_call(
        prepare_kernel,
        in_specs=[SMEM, VMEM],
        out_specs=[SMEM, VMEM],
        out_shape=[
            jax.ShapeDtypeStruct((SIZE,), jnp.int32),
            jax.ShapeDtypeStruct((8, 512, 512), jnp.bfloat16),
        ],
        compiler_params=pltpu.CompilerParams(vmem_limit_bytes=LIMIT),
        name="prepare",
    )(table, superop)
    blocks = exchange(blocks.reshape(128, 64, 128))
    blocks = pl.pallas_call(
        first_kernel,
        in_specs=[SMEM, HBM, VMEM],
        out_specs=VMEM,
        out_shape=jax.ShapeDtypeStruct((8192, 128), jnp.float32),
        scratch_shapes=[BUFFER, BUFFER, MATRICES, pltpu.SemaphoreType.DMA],
        compiler_params=pltpu.CompilerParams(vmem_limit_bytes=LIMIT),
        name="first",
    )(table, matrices, blocks.reshape(8192, 128))
    blocks = exchange(blocks.reshape(128, 64, 128))
    device = lax.axis_index(AX).astype(jnp.int32).reshape(1)
    tiles, trace = pl.pallas_call(
        second_kernel,
        in_specs=[SMEM, SMEM, HBM, VMEM],
        out_specs=[VMEM, SMEM],
        out_shape=[
            jax.ShapeDtypeStruct((8192, 128), jnp.float32),
            jax.ShapeDtypeStruct((1, 1), jnp.float32),
        ],
        scratch_shapes=[BUFFER, BUFFER, MATRICES, pltpu.SemaphoreType.DMA],
        compiler_params=pltpu.CompilerParams(vmem_limit_bytes=LIMIT),
        name="second",
    )(table, device, matrices, blocks.reshape(8192, 128))
    rho_out = tiles.reshape(2, 8, 64, 8, 128).transpose(0, 1, 3, 2, 4).reshape(2, 64, 8192)
    parts = exchange(jnp.broadcast_to(trace[0, 0], (128, 1, 128)))
    return rho_out, jnp.sum(parts[:, 0, 0]) / ROWS


def solution(mesh):
    spec = P(None, AX, None)
    return jax.shard_map(
        per_device, mesh=mesh, in_specs=(spec, P(), P()), out_specs=(spec, P()), check_vma=False
    )
```

```python
import jax
import jax.numpy as jnp
from jax import lax
from jax.experimental import pallas as pl
from jax.experimental.pallas import tpu as pltpu
from jax.sharding import PartitionSpec as P

ROWS = 8192
AX = ("hi", "grp")
RI = 13

W = 0
WINV = 16
U = 32
S0 = 48
A2 = 80
C2 = 112
P1 = 176
SC = 208
RARE = 220
G = 224
OCCL = 320
OCCT = 328
OCCR = 336
SUBC = 344
TMP = 352
OCC = 384
USED = 400
SIZE = 432


def pick(cond, a, b):
    return jnp.where(cond, jnp.int32(a), jnp.int32(b))


def lane_of(T, lanes, x):
    lane = jnp.int32(0)
    for p in range(7):
        lane = pick(T[lanes + p] == x, p, lane)
    return lane


def other_lanes(T, base, taken):
    for p in range(7):
        T[TMP + p] = jnp.int32(0)
    for lane in taken:
        T[TMP + lane] = jnp.int32(1)
    for k in range(4):
        free = jnp.int32(0)
        for p in range(7):
            free = pick(T[TMP + p] == 0, p, free)
        T[TMP + free] = jnp.int32(1)
        T[base + 5 + k] = free


def fill_slots(T, base, done, slots=10):
    for k in range(slots):
        free = jnp.int32(0)
        for s in range(slots):
            free = pick(T[USED + s] == 0, s, free)
        if k < done:
            free = jnp.where(T[base + k] >= 0, T[base + k], free)
        T[USED + free] = jnp.int32(1)
        T[base + k] = free


def set_strides(T, base, target):
    for k in range(10):
        s = T[base + k]
        T[base + k] = jnp.left_shift(jnp.int32(1), s)
        T[base + 10 + k] = jnp.left_shift(jnp.int32(1), T[target + s])


def make_plan_0(perm, T):
    one = jnp.int32(1)
    for q in range(13):
        w = perm[0, perm[1, q]]
        T[W + q] = w
        T[WINV + w] = jnp.int32(q)
    for b in range(16):
        T[TMP + b] = jnp.int32(0)
        T[USED + b] = jnp.int32(0)
    for q in range(4):
        T[TMP + T[W + q]] = jnp.int32(2)
    for j in range(4):
        T[U + j] = perm[0, j]
        T[TMP + perm[0, j]] = one
    for _ in range(2):
        x = jnp.int32(0)
        for b in range(12, -1, -1):
            x = pick(T[TMP + b] == 0, b, x)
        T[TMP + x] = one
    for s in range(10):
        T[OCC + s] = jnp.int32(3 + s)
    for i in range(3):
        best = jnp.int32(-1)
        for s in range(10):
            good = jnp.logical_and(T[TMP + 3 + s] == 1, T[USED + s] == 0)
            best = pick(good, s, best)
        slot = jnp.where(T[TMP + i] == 1, -1, best)
        active = slot >= 0
        safe = jnp.maximum(slot, 0)
        T[USED + safe] = jnp.where(active, one, T[USED + safe])
        T[OCCL + i] = jnp.where(active, slot + 3, jnp.int32(i))
        T[OCC + safe] = jnp.where(active, jnp.int32(i), T[OCC + safe])
        T[S0 + i] = slot
        T[S0 + 20 + i] = pick(active, 1 << i, 0)
    fill_slots(T, S0, 3)
    kept = jnp.int32(0)
    sent = jnp.int32(0)
    for s in range(10):
        occ = T[OCC + s]
        is_kept = T[TMP + occ] == 1
        T[USED + s] = jnp.where(is_kept, kept, sent + 3)
        T[jnp.where(is_kept, OCCL + 3 + kept, OCCT + sent)] = occ
        kept = jnp.where(is_kept, kept + 1, kept)
        sent = jnp.where(is_kept, sent, sent + 1)
    T[OCCL + 6] = jnp.int32(RI)
    set_strides(T, S0, USED)


def make_plan_1(T):
    one = jnp.int32(1)
    u = tuple(T[U + j] for j in range(4))
    for k in range(2):
        base = G + 20 * k
        lanes = [lane_of(T, OCCL, x) for x in (RI, u[2 * k], u[2 * k + 1])]
        other_lanes(T, base, lanes)
        for p in range(3):
            T[base + p] = lanes[p]
        T[base + 3] = jnp.int32(7)
        T[base + 4] = jnp.int32(8)
    for b in range(16):
        T[TMP + b] = jnp.int32(0)
        T[USED + b] = jnp.int32(0)
    for j in range(4):
        T[TMP + u[j]] = one
    for s in range(10):
        T[OCC + s] = jnp.int32(3 + s)
    for i in range(3):
        mine_u = T[TMP + i]
        mine_ok = jnp.logical_and(mine_u == 0, T[WINV + i] < 6)
        best = jnp.int32(-1)
        spare = jnp.int32(-1)
        for b in range(3, 13):
            free = jnp.logical_and(T[TMP + b] == 0, T[USED + b - 3] == 0)
            spare = pick(free, b, spare)
            best = pick(jnp.logical_and(free, T[WINV + b] < 6), b, best)
        other = jnp.where(mine_u == 0, -1, spare)
        bit = jnp.where(mine_ok, -1, jnp.where(best >= 0, best, other))
        active = bit >= 0
        safe = jnp.maximum(bit, 3)
        T[USED + safe - 3] = jnp.where(active, one, T[USED + safe - 3])
        T[P1 + i] = jnp.where(active, bit - 3, -1)
        T[OCCR + i] = jnp.where(active, bit, jnp.int32(i))
        T[OCC + safe - 3] = jnp.where(active, jnp.int32(i), T[OCC + safe - 3])
        T[P1 + 20 + i] = pick(active, 1 << i, 0)
    fill_slots(T, P1, 3)
    rare = jnp.int32(0)
    rare_amt = jnp.int32(0)
    rare_q = jnp.int32(6)
    for i in range(3):
        q = T[WINV + T[OCCR + i]]
        bad = q >= 6
        rare = pick(bad, 1, rare)
        rare_amt = pick(bad, 1 << i, rare_amt)
        rare_q = jnp.where(bad, q, rare_q)
    other = jnp.int32(0)
    kept = jnp.int32(0)
    rare_bit = jnp.int32(0)
    for s in range(10):
        occ = T[OCC + s]
        in_u = jnp.int32(-1)
        for j in range(4):
            in_u = pick(occ == u[j], 6 + j, in_u)
        place = jnp.where(in_u >= 0, in_u, other)
        other = jnp.where(in_u >= 0, other, other + 1)
        T[TMP + s] = place
        q = T[WINV + occ]
        is_kept = q < 6
        fits = kept < 3
        bit = jnp.where(is_kept, jnp.where(fits, kept, rare_q - 3), q - 3)
        slot = jnp.where(jnp.logical_and(is_kept, fits), kept, 3)
        T[OCCR + 3 + slot] = jnp.where(is_kept, occ, jnp.int32(RI))
        rare_bit = jnp.where(jnp.logical_and(is_kept, jnp.logical_not(fits)), occ, rare_bit)
        kept = jnp.where(is_kept, kept + 1, kept)
        T[SC + place] = jnp.left_shift(one, bit)
    for i in range(3):
        q = T[WINV + T[OCCR + i]]
        T[OCCR + i] = jnp.where(q >= 6, rare_bit, T[OCCR + i])
    T[OCCR + 6] = jnp.int32(RI)
    T[RARE] = rare
    T[RARE + 1] = jnp.left_shift(one, rare_q - 3)
    T[RARE + 2] = rare_amt
    set_strides(T, P1, TMP)


def make_plan_2(T):
    one = jnp.int32(1)
    w = tuple(T[W + q] for q in range(13))
    for k in range(3):
        T[SUBC + k] = T[OCCL + k]
        T[OCC + k] = T[OCCL + 3 + k]
    for k in range(7):
        T[OCC + 3 + k] = T[OCCT + k]
    for s in range(16):
        T[USED + s] = jnp.int32(0)
    for i in range(3):
        mine = T[SUBC + i]
        best = jnp.int32(-1)
        for s in range(10):
            good = jnp.logical_and(T[WINV + T[OCC + s]] >= 4, T[USED + s] == 0)
            best = pick(good, s, best)
        slot = jnp.where(T[WINV + mine] >= 4, -1, best)
        active = slot >= 0
        safe = jnp.maximum(slot, 0)
        T[USED + safe] = jnp.where(active, one, T[USED + safe])
        new = T[OCC + safe]
        T[SUBC + i] = jnp.where(active, new, mine)
        T[OCC + safe] = jnp.where(active, mine, new)
        T[A2 + i] = slot
        T[A2 + 20 + i] = pick(active, 1 << i, 0)
    fill_slots(T, A2, 3)
    other = jnp.int32(0)
    for s in range(10):
        q = T[WINV + T[OCC + s]]
        T[TMP + s] = jnp.where(q < 4, q + 6, other)
        other = jnp.where(q < 4, other, other + 1)
    set_strides(T, A2, TMP)
    for s in range(10):
        T[USED + T[TMP + s]] = T[OCC + s]
    for s in range(10):
        T[OCC + s] = T[USED + s]
    rows = [lane_of(T, OCCR, w[q]) for q in range(6)]
    ri = lane_of(T, OCCR, RI)
    other_lanes(T, G + 40, (ri, rows[0], rows[1]))
    for k, v in enumerate((ri, 7, 8, rows[0], rows[1])):
        T[G + 40 + k] = jnp.int32(v)
    for k, v in enumerate((ri, 7, 8, rows[2], rows[3], rows[0], rows[1], rows[4], rows[5])):
        T[G + 60 + k] = jnp.int32(v)
    for k, v in enumerate((6, 7, 8, 2, 3, 0, 1, 4, 5)):
        T[G + 69 + k] = jnp.int32(v)
    for i in range(3):
        T[OCC + 6 + i] = T[SUBC + i]
    for s in range(10):
        T[TMP + s] = T[WINV + T[OCC + s]] - 7
    for k in range(10):
        slot = jnp.int32(0)
        for s in range(10):
            slot = pick(T[OCC + s] == w[3 + k], s, slot)
        T[C2 + k] = slot
        if k < 4:
            T[TMP + slot] = jnp.int32(6 + k)
    set_strides(T, C2, TMP)


def sums(start, strides):
    out = [start]
    for stride in strides:
        out = out + [o + stride for o in out]
    return out


def block_loop(src, dst, load, store, work, first=0, last=32):
    src_low = sums(jnp.int32(0), src[:3])
    dst_low = sums(jnp.int32(0), dst[:3])

    def block(b, carry):
        src_base = jnp.int32(0)
        dst_base = jnp.int32(0)
        for k in range(5):
            bit = jnp.bitwise_and(jnp.right_shift(b, k), 1)
            src_base = src_base + bit * src[5 + k]
            dst_base = dst_base + bit * dst[5 + k]
        vs = []
        for high in sums(src_base, src[3:5]):
            vs.extend(load[tile_rows(high + low), :] for low in src_low)
        vs = work(vs)
        m = 0
        for high in sums(dst_base, dst[3:5]):
            for low in dst_low:
                store[tile_rows(high + low), :] = vs[m]
                m += 1
        return carry

    lax.fori_loop(first, last, block, 0)


def table_strides(T, base):
    return [T[base + k] * 8 for k in range(10)], [T[base + 10 + k] * 8 for k in range(10)]


def sublane_swaps(src, dst, load, store, amounts):
    sub = lax.broadcasted_iota(jnp.int32, (8, 128), 0)
    hits = [jnp.bitwise_and(sub, amount) for amount in amounts]
    keep_x = [hit == 0 for hit in hits]
    keep_y = [hit == amount for hit, amount in zip(hits, amounts)]

    def work(vs):
        for k in range(3):
            for m in range(32):
                if not m >> k & 1:
                    n = m | 1 << k
                    x, y = vs[m], vs[n]
                    vs[m] = jnp.where(keep_x[k], x, pltpu.roll(y, 1 << k, 0))
                    vs[n] = jnp.where(keep_y[k], y, pltpu.roll(x, 8 - (1 << k), 0))
        return vs

    block_loop(src, dst, load, store, work)


def table_swaps(T, base, load, store):
    src, dst = table_strides(T, base)
    sublane_swaps(src, dst, load, store, [T[base + 20 + k] for k in range(3)])


def transposes(T, base, load, store, first, last):
    src, dst = table_strides(T, base)

    def work(vs):
        out = []
        for half in range(2):
            y = jnp.concatenate(vs[16 * half : 16 * half + 16], axis=0).T
            out.extend(y[8 * m : 8 * m + 8, :] for m in range(16))
        return out

    block_loop(src, dst, load, store, work, first, last)


def turn(hbm, src, dst, sems):
    low = lax.broadcasted_iota(jnp.int32, (64, 128), 1) < 64

    def copies(c):
        out = []
        for half in range(2):
            rows = pl.ds(pl.multiple_of(half * 4096 + c * 256, 256), 256)
            out.append(pltpu.make_async_copy(hbm.at[rows], src.at[rows], sems.at[half, c]))
        return out

    for c in range(16):
        for copy in copies(c):
            copy.start()

    def body(c, carry):
        for copy in copies(c):
            copy.wait()
        for k in range(4):
            rows = [pl.ds(pl.multiple_of(half * 4096 + c * 256 + k * 64, 64), 64) for half in range(2)]
            y = jnp.concatenate([src[r, :] for r in rows], axis=0).T
            p, q = y[:64, :], y[64:, :]
            moved = pltpu.roll(jnp.where(low, q, p), 64, 1)
            dst[rows[0], :] = jnp.where(low, p, moved)
            dst[rows[1], :] = jnp.where(low, moved, q)
        return carry

    lax.fori_loop(0, 16, body, 0)


def tile_rows(row):
    return pl.ds(pl.multiple_of(row, 8), 8)


def build_matrix(T, base, out_base, sup, gh_ref, gl_ref):
    real, imag = sup[0], sup[1]
    top = jnp.concatenate([real, -imag], axis=1)
    bottom = jnp.concatenate([imag, real], axis=1)
    kern = jnp.concatenate([top, bottom], axis=0)
    index_i = lax.broadcasted_iota(jnp.int32, (512, 32), 0)
    index_o = lax.broadcasted_iota(jnp.int32, (32, 512), 1)

    def code(index, start, first, count):
        total = jnp.zeros_like(index)
        place = {0: 4, 1: 0, 2: 1, 3: 2, 4: 3}
        for k in range(first, first + count):
            bit = jnp.bitwise_and(jnp.right_shift(index, T[start + k]), 1)
            total = total + jnp.left_shift(bit, place[k] if first == 0 else k - first)
        return total

    one_i = (code(index_i, base, 0, 5) == lax.broadcasted_iota(jnp.int32, (512, 32), 1)).astype(jnp.bfloat16)
    one_o = (code(index_o, out_base, 0, 5) == lax.broadcasted_iota(jnp.int32, (32, 512), 0)).astype(jnp.bfloat16)
    rest_i = code(lax.broadcasted_iota(jnp.int32, (512, 128), 0), base, 5, 4)
    rest_o = code(lax.broadcasted_iota(jnp.int32, (8, 512), 1), out_base, 5, 4)
    same = jnp.concatenate([rest_i] * 4, axis=1) == jnp.concatenate([rest_o] * 64, axis=0)
    kh = kern.astype(jnp.bfloat16)
    kl = (kern - kh.astype(jnp.float32)).astype(jnp.bfloat16)
    for part, ref in ((kh, gh_ref), (kl, gl_ref)):
        left = lax.dot_general(one_i, part, (((1,), (1,)), ((), ())), preferred_element_type=jnp.float32)
        full = jnp.dot(left.astype(jnp.bfloat16), one_o, preferred_element_type=jnp.float32)
        ref[...] = jnp.where(same, full, 0.0).astype(jnp.bfloat16)


def mix(parts, gh, gl):
    x = jnp.concatenate(parts, axis=1)
    xh = x.astype(jnp.bfloat16)
    xl = (x - xh.astype(jnp.float32)).astype(jnp.bfloat16)
    y = jnp.dot(xl, gh, preferred_element_type=jnp.float32)
    y = y + jnp.dot(xh, gl, preferred_element_type=jnp.float32)
    return y + jnp.dot(xh, gh, preferred_element_type=jnp.float32)


def split_kernel(perm, rho, out, T, buf):
    step = pl.program_id(0)

    @pl.when(step == 0)
    def _():
        make_plan_0(perm, T)

    for c in range(8):
        lanes = slice(c * 128, c * 128 + 128)
        x = jnp.concatenate([rho[0, :, lanes], rho[1, :, lanes]], axis=0)
        buf[pl.ds(pl.multiple_of(step * 1024 + c * 128, 128), 128), :] = x.T

    @pl.when(step == 7)
    def _():
        table_swaps(T, S0, buf, out)


def prepare_kernel(first_table, sup, T, matrices):
    def copy(k, carry):
        T[k] = first_table[k]
        return carry

    lax.fori_loop(0, TMP, copy, 0)
    make_plan_1(T)
    make_plan_2(T)
    for k, (base, out_base) in enumerate(((G, G), (G + 20, G + 20), (G + 40, G + 40), (G + 60, G + 69))):
        build_matrix(T, base, out_base, sup[k // 2], matrices.at[2 * k], matrices.at[2 * k + 1])


def mix_pass(src, dst, matrices, step, store=None):
    def body(g, carry):
        first = g * 4 if step == 1 else g
        rows = [pl.ds(pl.multiple_of((first + step * j) * 512, 512), 512) for j in range(4)]
        y = mix([src[r, :] for r in rows], matrices[0], matrices[1])
        for j in range(4):
            piece = y[:, j * 128 : (j + 1) * 128]
            if store is None:
                dst[rows[j], :] = piece
            else:
                store(g, j, piece)
        return carry

    lax.fori_loop(0, 4, body, 0)


def first_kernel(T, matrices_hbm, x, out, buf, buf2, matrices, sem, sems):
    fetch = pltpu.make_async_copy(matrices_hbm.at[pl.ds(0, 4)], matrices, sem)
    fetch.start()
    turn(x, buf2, buf, sems)
    table_swaps(T, P1, buf, buf2)
    fetch.wait()
    mix_pass(buf2, buf2, matrices.at[pl.ds(0, 2)], 1)
    strides = [T[SC + k] * 8 for k in range(10)]
    low = [jnp.int32(0)]
    for k in range(3):
        low = low + [o + strides[k] for o in low]

    def scatter(h, j, piece):
        start = jnp.bitwise_and(h, 1) * strides[6] + jnp.right_shift(h, 1) * strides[7]
        if j & 1:
            start = start + strides[8]
        if j & 2:
            start = start + strides[9]
        high = [start]
        for k in range(3, 6):
            high = high + [o + strides[k] for o in high]
        for n in range(64):
            out[tile_rows(high[n >> 3] + low[n & 7]), :] = piece[n * 8 : n * 8 + 8, :]

    mix_pass(buf2, None, matrices.at[pl.ds(2, 2)], 4, scatter)

    @pl.when(T[RARE] == 1)
    def _():
        stride = T[RARE + 1]
        amount = T[RARE + 2]
        sub = lax.broadcasted_iota(jnp.int32, (8, 128), 0)
        hit = jnp.bitwise_and(sub, amount)

        def pair(b, carry):
            low = jnp.bitwise_and(b, stride - 1)
            t = (b - low) * 2 + low
            a_rows, b_rows = tile_rows(t * 8), tile_rows((t + stride) * 8)
            a, c = out[a_rows, :], out[b_rows, :]
            up = pltpu.roll(c, amount, 0)
            down = pltpu.roll(a, 8 - amount, 0)
            out[a_rows, :] = jnp.where(hit == 0, a, up)
            out[b_rows, :] = jnp.where(hit == amount, c, down)
            return carry

        lax.fori_loop(0, 512, pair, 0)


def second_kernel(T, matrices_hbm, x, out, buf, buf2, matrices, sem, sems):
    fetch = pltpu.make_async_copy(matrices_hbm.at[pl.ds(4, 4)], matrices, sem)
    fetch.start()
    turn(x, buf2, buf, sems)
    table_swaps(T, A2, buf, buf2)
    fetch.wait()
    mix_pass(buf2, buf, matrices.at[pl.ds(0, 2)], 1)
    mix_pass(buf, buf2, matrices.at[pl.ds(2, 2)], 4)
    slots = [8 << k for k in (6, 7, 8, 0, 1, 2, 3, 4, 5, 9)]
    sublane_swaps(slots, slots, buf2, buf, (1, 2, 4))
    tiles = buf2.reshape(16, 512, 128)
    sends = []
    for c in range(4):
        transposes(T, C2, buf, buf2, 8 * c, 8 * c + 8)
        part = pl.ds(c * 128, 128)
        sends.append(pltpu.make_async_copy(tiles.at[:, part], out.at[:, part], sems.at[0, c]))
        sends[-1].start()
    for send in sends:
        send.wait()


def trace_kernel(T, pos, sup, x, out):
    step = pl.program_id(0)
    lane = lax.broadcasted_iota(jnp.int32, (8, 128), 1)
    sub = lax.broadcasted_iota(jnp.int32, (8, 128), 0)

    def bit_at(index, k, place):
        return jnp.left_shift(jnp.bitwise_and(jnp.right_shift(index, k), 1), place)

    col_base = jnp.int32(0)
    for k in range(7):
        col_base = col_base + bit_at(pos[0], k, T[WINV + T[OCCT + k]])
    col = jnp.zeros_like(lane) + col_base
    for k in range(6):
        col = col + bit_at(lane, k, T[WINV + T[OCCL + k]])
    row_sub = jnp.zeros_like(sub)
    for k in range(3):
        row_sub = row_sub + bit_at(sub, k, T[WINV + T[OCCR + k]])
    row_places = [T[WINV + T[OCCR + 3 + k]] for k in range(3)]
    tables = []
    for pair in range(2):
        v = jnp.bitwise_and(jnp.right_shift(col, 2 * pair), 3)
        for part in range(2):
            for a in range(4):
                value = jnp.zeros((8, 128), jnp.float32)
                for b in range(4):
                    index = 4 * a + b
                    total = sup[part, 0, index] + sup[part, 5, index]
                    total = total + sup[part, 10, index] + sup[part, 15, index]
                    value = jnp.where(v == b, total, value)
                tables.append(value)
    imag = lane >= 64
    high = jnp.right_shift(col, 4)

    def tile(n, total):
        g = step * 64 + n
        row = jnp.right_shift(g, 3) * 64
        for k in range(3):
            row = row + bit_at(g, k, row_places[k])
        row = row_sub + row
        factors = []
        for pair in range(2):
            u = jnp.bitwise_and(jnp.right_shift(row, 2 * pair), 3)
            for part in range(2):
                value = tables[8 * pair + 4 * part]
                for a in range(1, 4):
                    value = jnp.where(u == a, tables[8 * pair + 4 * part + a], value)
                factors.append(value)
        r0, i0, r1, i1 = factors
        weight = jnp.where(imag, -(r0 * i1 + i0 * r1), r0 * r1 - i0 * i1)
        data = x[tile_rows(n * 8), :]
        return total + jnp.where(jnp.right_shift(row, 4) == high, weight * data, 0.0)

    total = lax.fori_loop(0, 64, tile, jnp.zeros((8, 128), jnp.float32), unroll=4)

    @pl.when(step == 0)
    def _():
        out[0, 0] = jnp.float32(0.0)

    out[0, 0] = out[0, 0] + jnp.sum(total)


SMEM = pl.BlockSpec(memory_space=pltpu.SMEM)
VMEM = pl.BlockSpec(memory_space=pltpu.VMEM)
HBM = pl.BlockSpec(memory_space=pl.ANY)
LIMIT = 60 << 20
BUFFER = pltpu.VMEM((8192, 128), jnp.float32)
MATRICES = pltpu.VMEM((4, 512, 512), jnp.bfloat16)
SCRATCH = [BUFFER, BUFFER, MATRICES, pltpu.SemaphoreType.DMA, pltpu.SemaphoreType.DMA((2, 16))]


def exchange(blocks):
    return lax.all_to_all(blocks, AX, split_axis=0, concat_axis=0, tiled=True)


def per_device(rho, perm, superop):
    blocks, table = pl.pallas_call(
        split_kernel,
        grid=(8,),
        in_specs=[SMEM, pl.BlockSpec((2, 64, 1024), lambda i: (0, 0, i))],
        out_specs=[pl.BlockSpec((8192, 128), lambda i: (0, 0)), SMEM],
        scratch_shapes=[BUFFER],
        out_shape=[
            jax.ShapeDtypeStruct((8192, 128), jnp.float32),
            jax.ShapeDtypeStruct((SIZE,), jnp.int32),
        ],
        compiler_params=pltpu.CompilerParams(vmem_limit_bytes=LIMIT),
        name="split",
    )(perm, rho)
    table, matrices = pl.pallas_call(
        prepare_kernel,
        in_specs=[SMEM, VMEM],
        out_specs=[SMEM, VMEM],
        out_shape=[
            jax.ShapeDtypeStruct((SIZE,), jnp.int32),
            jax.ShapeDtypeStruct((8, 512, 512), jnp.bfloat16),
        ],
        compiler_params=pltpu.CompilerParams(vmem_limit_bytes=LIMIT),
        name="prepare",
    )(table, superop)
    blocks = exchange(blocks.reshape(128, 64, 128))
    blocks = pl.pallas_call(
        first_kernel,
        in_specs=[SMEM, HBM, HBM],
        out_specs=VMEM,
        out_shape=jax.ShapeDtypeStruct((8192, 128), jnp.float32),
        scratch_shapes=SCRATCH,
        compiler_params=pltpu.CompilerParams(vmem_limit_bytes=LIMIT),
        name="first",
    )(table, matrices, blocks.reshape(8192, 128))
    device = lax.axis_index(AX).astype(jnp.int32).reshape(1)
    trace = pl.pallas_call(
        trace_kernel,
        grid=(16,),
        in_specs=[SMEM, SMEM, SMEM, pl.BlockSpec((512, 128), lambda i: (i, 0))],
        out_specs=SMEM,
        out_shape=jax.ShapeDtypeStruct((1, 1), jnp.float32),
        name="trace",
    )(table, device, superop[1], blocks)
    blocks = exchange(blocks.reshape(128, 64, 128))
    blocks, trace = lax.optimization_barrier((blocks, trace))
    parts = exchange(jnp.broadcast_to(trace[0, 0], (128, 1, 128)))
    tiles = pl.pallas_call(
        second_kernel,
        in_specs=[SMEM, HBM, HBM],
        out_specs=HBM,
        out_shape=jax.ShapeDtypeStruct((16, 512, 128), jnp.float32),
        scratch_shapes=SCRATCH,
        compiler_params=pltpu.CompilerParams(vmem_limit_bytes=LIMIT),
        name="second",
    )(table, matrices, blocks.reshape(8192, 128))
    rho_out = tiles.reshape(2, 8, 64, 8, 128).transpose(0, 1, 3, 2, 4).reshape(2, 64, 8192)
    return rho_out, jnp.sum(parts[:, 0, 0]) / ROWS


def solution(mesh):
    spec = P(None, AX, None)
    return jax.shard_map(
        per_device, mesh=mesh, in_specs=(spec, P(), P()), out_specs=(spec, P()), check_vma=False
    )
```

```python
import jax
import jax.numpy as jnp
from jax import lax
from jax.experimental import pallas as pl
from jax.experimental.pallas import tpu as pltpu
from jax.sharding import PartitionSpec as P

ROWS = 8192
AX = ("hi", "grp")
RI = 13

W = 0
WINV = 16
U = 32
S0 = 48
A2 = 80
C2 = 112
P1 = 176
SC = 208
RARE = 220
G = 224
OCCL = 320
OCCT = 328
OCCR = 336
SUBC = 344
TMP = 352
OCC = 384
USED = 400
SIZE = 432


def pick(cond, a, b):
    return jnp.where(cond, jnp.int32(a), jnp.int32(b))


def lane_of(T, lanes, x):
    lane = jnp.int32(0)
    for p in range(7):
        lane = pick(T[lanes + p] == x, p, lane)
    return lane


def other_lanes(T, base, taken):
    for p in range(7):
        T[TMP + p] = jnp.int32(0)
    for lane in taken:
        T[TMP + lane] = jnp.int32(1)
    for k in range(4):
        free = jnp.int32(0)
        for p in range(7):
            free = pick(T[TMP + p] == 0, p, free)
        T[TMP + free] = jnp.int32(1)
        T[base + 5 + k] = free


def fill_slots(T, base, done, slots=10):
    for k in range(slots):
        free = jnp.int32(0)
        for s in range(slots):
            free = pick(T[USED + s] == 0, s, free)
        if k < done:
            free = jnp.where(T[base + k] >= 0, T[base + k], free)
        T[USED + free] = jnp.int32(1)
        T[base + k] = free


def set_strides(T, base, target):
    for k in range(10):
        s = T[base + k]
        T[base + k] = jnp.left_shift(jnp.int32(1), s)
        T[base + 10 + k] = jnp.left_shift(jnp.int32(1), T[target + s])


def make_plan_0(perm, T):
    one = jnp.int32(1)
    for q in range(13):
        w = perm[0, perm[1, q]]
        T[W + q] = w
        T[WINV + w] = jnp.int32(q)
    for b in range(16):
        T[TMP + b] = jnp.int32(0)
        T[USED + b] = jnp.int32(0)
    for q in range(4):
        T[TMP + T[W + q]] = jnp.int32(2)
    for j in range(4):
        T[U + j] = perm[0, j]
        T[TMP + perm[0, j]] = one
    for _ in range(2):
        x = jnp.int32(0)
        for b in range(12, -1, -1):
            x = pick(T[TMP + b] == 0, b, x)
        T[TMP + x] = one
    for s in range(10):
        T[OCC + s] = jnp.int32(3 + s)
    for i in range(3):
        best = jnp.int32(-1)
        for s in range(10):
            good = jnp.logical_and(T[TMP + 3 + s] == 1, T[USED + s] == 0)
            best = pick(good, s, best)
        slot = jnp.where(T[TMP + i] == 1, -1, best)
        active = slot >= 0
        safe = jnp.maximum(slot, 0)
        T[USED + safe] = jnp.where(active, one, T[USED + safe])
        T[OCCL + i] = jnp.where(active, slot + 3, jnp.int32(i))
        T[OCC + safe] = jnp.where(active, jnp.int32(i), T[OCC + safe])
        T[S0 + i] = slot
        T[S0 + 20 + i] = pick(active, 1 << i, 0)
    for k in range(10):
        free = jnp.int32(0)
        best = jnp.int32(-1)
        for s in range(10):
            unused = T[USED + s] == 0
            free = pick(unused, s, free)
            best = pick(jnp.logical_and(unused, T[TMP + T[OCC + s]] == 1), s, best)
        free = jnp.where(best >= 0, best, free)
        if k < 3:
            free = jnp.where(T[S0 + k] >= 0, T[S0 + k], free)
        T[USED + free] = one
        T[S0 + k] = free
    kept = jnp.int32(0)
    sent = jnp.int32(0)
    for k in range(10):
        s = T[S0 + k]
        occ = T[OCC + s]
        is_kept = T[TMP + occ] == 1
        T[USED + s] = jnp.where(is_kept, kept, sent + 3)
        T[jnp.where(is_kept, OCCL + 3 + kept, OCCT + sent)] = occ
        kept = jnp.where(is_kept, kept + 1, kept)
        sent = jnp.where(is_kept, sent, sent + 1)
    T[OCCL + 6] = jnp.int32(RI)
    set_strides(T, S0, USED)


def make_plan_1(T):
    one = jnp.int32(1)
    u = tuple(T[U + j] for j in range(4))
    for k in range(2):
        base = G + 20 * k
        lanes = [lane_of(T, OCCL, x) for x in (RI, u[2 * k], u[2 * k + 1])]
        other_lanes(T, base, lanes)
        for p in range(3):
            T[base + p] = lanes[p]
        T[base + 3] = jnp.int32(7)
        T[base + 4] = jnp.int32(8)
    for b in range(16):
        T[TMP + b] = jnp.int32(0)
        T[USED + b] = jnp.int32(0)
    for j in range(4):
        T[TMP + u[j]] = one
    for s in range(10):
        T[OCC + s] = jnp.int32(3 + s)
    for i in range(3):
        mine_u = T[TMP + i]
        mine_ok = jnp.logical_and(mine_u == 0, T[WINV + i] < 6)
        best = jnp.int32(-1)
        spare = jnp.int32(-1)
        for b in range(3, 13):
            free = jnp.logical_and(T[TMP + b] == 0, T[USED + b - 3] == 0)
            spare = pick(free, b, spare)
            best = pick(jnp.logical_and(free, T[WINV + b] < 6), b, best)
        other = jnp.where(mine_u == 0, -1, spare)
        bit = jnp.where(mine_ok, -1, jnp.where(best >= 0, best, other))
        active = bit >= 0
        safe = jnp.maximum(bit, 3)
        T[USED + safe - 3] = jnp.where(active, one, T[USED + safe - 3])
        T[P1 + i] = jnp.where(active, bit - 3, -1)
        T[OCCR + i] = jnp.where(active, bit, jnp.int32(i))
        T[OCC + safe - 3] = jnp.where(active, jnp.int32(i), T[OCC + safe - 3])
        T[P1 + 20 + i] = pick(active, 1 << i, 0)
    fill_slots(T, P1, 3)
    rare = jnp.int32(0)
    rare_amt = jnp.int32(0)
    rare_q = jnp.int32(6)
    for i in range(3):
        q = T[WINV + T[OCCR + i]]
        bad = q >= 6
        rare = pick(bad, 1, rare)
        rare_amt = pick(bad, 1 << i, rare_amt)
        rare_q = jnp.where(bad, q, rare_q)
    other = jnp.int32(0)
    kept = jnp.int32(0)
    rare_bit = jnp.int32(0)
    for s in range(10):
        occ = T[OCC + s]
        in_u = jnp.int32(-1)
        for j in range(4):
            in_u = pick(occ == u[j], 6 + j, in_u)
        place = jnp.where(in_u >= 0, in_u, other)
        other = jnp.where(in_u >= 0, other, other + 1)
        T[TMP + s] = place
        q = T[WINV + occ]
        is_kept = q < 6
        fits = kept < 3
        bit = jnp.where(is_kept, jnp.where(fits, kept, rare_q - 3), q - 3)
        slot = jnp.where(jnp.logical_and(is_kept, fits), kept, 3)
        T[OCCR + 3 + slot] = jnp.where(is_kept, occ, jnp.int32(RI))
        rare_bit = jnp.where(jnp.logical_and(is_kept, jnp.logical_not(fits)), occ, rare_bit)
        kept = jnp.where(is_kept, kept + 1, kept)
        T[SC + place] = jnp.left_shift(one, bit)
    for i in range(3):
        q = T[WINV + T[OCCR + i]]
        T[OCCR + i] = jnp.where(q >= 6, rare_bit, T[OCCR + i])
    T[OCCR + 6] = jnp.int32(RI)
    T[RARE] = rare
    T[RARE + 1] = jnp.left_shift(one, rare_q - 3)
    T[RARE + 2] = rare_amt
    set_strides(T, P1, TMP)


def make_plan_2(T):
    one = jnp.int32(1)
    w = tuple(T[W + q] for q in range(13))
    for k in range(3):
        T[SUBC + k] = T[OCCL + k]
        T[OCC + k] = T[OCCL + 3 + k]
    for k in range(7):
        T[OCC + 3 + k] = T[OCCT + k]
    for s in range(16):
        T[USED + s] = jnp.int32(0)
    for i in range(3):
        mine = T[SUBC + i]
        best = jnp.int32(-1)
        for s in range(10):
            good = jnp.logical_and(T[WINV + T[OCC + s]] >= 4, T[USED + s] == 0)
            best = pick(good, s, best)
        slot = jnp.where(T[WINV + mine] >= 4, -1, best)
        active = slot >= 0
        safe = jnp.maximum(slot, 0)
        T[USED + safe] = jnp.where(active, one, T[USED + safe])
        new = T[OCC + safe]
        T[SUBC + i] = jnp.where(active, new, mine)
        T[OCC + safe] = jnp.where(active, mine, new)
        T[A2 + i] = slot
        T[A2 + 20 + i] = pick(active, 1 << i, 0)
    fill_slots(T, A2, 3)
    other = jnp.int32(0)
    for s in range(10):
        q = T[WINV + T[OCC + s]]
        T[TMP + s] = jnp.where(q < 4, q + 6, other)
        other = jnp.where(q < 4, other, other + 1)
    set_strides(T, A2, TMP)
    for s in range(10):
        T[USED + T[TMP + s]] = T[OCC + s]
    for s in range(10):
        T[OCC + s] = T[USED + s]
    rows = [lane_of(T, OCCR, w[q]) for q in range(6)]
    ri = lane_of(T, OCCR, RI)
    other_lanes(T, G + 40, (ri, rows[0], rows[1]))
    for k, v in enumerate((ri, 7, 8, rows[0], rows[1])):
        T[G + 40 + k] = jnp.int32(v)
    for k, v in enumerate((ri, 7, 8, rows[2], rows[3], rows[0], rows[1], rows[4], rows[5])):
        T[G + 60 + k] = jnp.int32(v)
    for k, v in enumerate((6, 7, 8, 2, 3, 0, 1, 4, 5)):
        T[G + 69 + k] = jnp.int32(v)
    for i in range(3):
        T[OCC + 6 + i] = T[SUBC + i]
    for s in range(10):
        T[TMP + s] = T[WINV + T[OCC + s]] - 7
    for k in range(10):
        slot = jnp.int32(0)
        for s in range(10):
            slot = pick(T[OCC + s] == w[3 + k], s, slot)
        T[C2 + k] = slot
        if k < 4:
            T[TMP + slot] = jnp.int32(6 + k)
    set_strides(T, C2, TMP)


def sums(start, strides):
    out = [start]
    for stride in strides:
        out = out + [o + stride for o in out]
    return out


def block_loop(src, dst, load, store, work, first=0, last=32):
    src_low = sums(jnp.int32(0), src[:3])
    dst_low = sums(jnp.int32(0), dst[:3])

    def block(b, carry):
        src_base = jnp.int32(0)
        dst_base = jnp.int32(0)
        for k in range(5):
            bit = jnp.bitwise_and(jnp.right_shift(b, k), 1)
            src_base = src_base + bit * src[5 + k]
            dst_base = dst_base + bit * dst[5 + k]
        vs = []
        for high in sums(src_base, src[3:5]):
            vs.extend(load[tile_rows(high + low), :] for low in src_low)
        vs = work(vs)
        m = 0
        for high in sums(dst_base, dst[3:5]):
            for low in dst_low:
                store[tile_rows(high + low), :] = vs[m]
                m += 1
        return carry

    lax.fori_loop(first, last, block, 0)


def table_strides(T, base):
    return [T[base + k] * 8 for k in range(10)], [T[base + 10 + k] * 8 for k in range(10)]


def sublane_swaps(src, dst, load, store, amounts, first=0, last=32):
    sub = lax.broadcasted_iota(jnp.int32, (8, 128), 0)
    hits = [jnp.bitwise_and(sub, amount) for amount in amounts]
    keep_x = [hit == 0 for hit in hits]
    keep_y = [hit == amount for hit, amount in zip(hits, amounts)]

    def work(vs):
        for k in range(3):
            for m in range(32):
                if not m >> k & 1:
                    n = m | 1 << k
                    x, y = vs[m], vs[n]
                    vs[m] = jnp.where(keep_x[k], x, pltpu.roll(y, 1 << k, 0))
                    vs[n] = jnp.where(keep_y[k], y, pltpu.roll(x, 8 - (1 << k), 0))
        return vs

    block_loop(src, dst, load, store, work, first, last)


def table_swaps(T, base, load, store, first=0, last=32):
    src, dst = table_strides(T, base)
    sublane_swaps(src, dst, load, store, [T[base + 20 + k] for k in range(3)], first, last)


def transposes(T, base, load, store, first, last):
    src, dst = table_strides(T, base)

    def work(vs):
        out = []
        for half in range(2):
            y = jnp.concatenate(vs[16 * half : 16 * half + 16], axis=0).T
            out.extend(y[8 * m : 8 * m + 8, :] for m in range(16))
        return out

    block_loop(src, dst, load, store, work, first, last)


def turn(hbm, src, dst, sems):
    low = lax.broadcasted_iota(jnp.int32, (64, 128), 1) < 64

    def copies(c):
        out = []
        for half in range(2):
            rows = pl.ds(pl.multiple_of(half * 4096 + c * 256, 256), 256)
            out.append(pltpu.make_async_copy(hbm.at[rows], src.at[rows], sems.at[half, c]))
        return out

    for c in range(16):
        for copy in copies(c):
            copy.start()

    def body(c, carry):
        for copy in copies(c):
            copy.wait()
        for k in range(4):
            rows = [pl.ds(pl.multiple_of(half * 4096 + c * 256 + k * 64, 64), 64) for half in range(2)]
            y = jnp.concatenate([src[r, :] for r in rows], axis=0).T
            p, q = y[:64, :], y[64:, :]
            moved = pltpu.roll(jnp.where(low, q, p), 64, 1)
            dst[rows[0], :] = jnp.where(low, p, moved)
            dst[rows[1], :] = jnp.where(low, moved, q)
        return carry

    lax.fori_loop(0, 16, body, 0)


def tile_rows(row):
    return pl.ds(pl.multiple_of(row, 8), 8)


def build_matrix(T, base, out_base, sup, gh_ref, gl_ref):
    real, imag = sup[0], sup[1]
    top = jnp.concatenate([real, -imag], axis=1)
    bottom = jnp.concatenate([imag, real], axis=1)
    kern = jnp.concatenate([top, bottom], axis=0)
    index_i = lax.broadcasted_iota(jnp.int32, (512, 32), 0)
    index_o = lax.broadcasted_iota(jnp.int32, (32, 512), 1)

    def code(index, start, first, count):
        total = jnp.zeros_like(index)
        place = {0: 4, 1: 0, 2: 1, 3: 2, 4: 3}
        for k in range(first, first + count):
            bit = jnp.bitwise_and(jnp.right_shift(index, T[start + k]), 1)
            total = total + jnp.left_shift(bit, place[k] if first == 0 else k - first)
        return total

    one_i = (code(index_i, base, 0, 5) == lax.broadcasted_iota(jnp.int32, (512, 32), 1)).astype(jnp.bfloat16)
    one_o = (code(index_o, out_base, 0, 5) == lax.broadcasted_iota(jnp.int32, (32, 512), 0)).astype(jnp.bfloat16)
    rest_i = code(lax.broadcasted_iota(jnp.int32, (512, 128), 0), base, 5, 4)
    rest_o = code(lax.broadcasted_iota(jnp.int32, (8, 512), 1), out_base, 5, 4)
    same = jnp.concatenate([rest_i] * 4, axis=1) == jnp.concatenate([rest_o] * 64, axis=0)
    kh = kern.astype(jnp.bfloat16)
    kl = (kern - kh.astype(jnp.float32)).astype(jnp.bfloat16)
    for part, ref in ((kh, gh_ref), (kl, gl_ref)):
        left = lax.dot_general(one_i, part, (((1,), (1,)), ((), ())), preferred_element_type=jnp.float32)
        full = jnp.dot(left.astype(jnp.bfloat16), one_o, preferred_element_type=jnp.float32)
        ref[...] = jnp.where(same, full, 0.0).astype(jnp.bfloat16)


def mix(parts, gh, gl):
    x = jnp.concatenate(parts, axis=1)
    xh = x.astype(jnp.bfloat16)
    xl = (x - xh.astype(jnp.float32)).astype(jnp.bfloat16)
    y = jnp.dot(xl, gh, preferred_element_type=jnp.float32)
    y = y + jnp.dot(xh, gl, preferred_element_type=jnp.float32)
    return y + jnp.dot(xh, gh, preferred_element_type=jnp.float32)


def split_kernel(perm, rho, out, T, x, buf, buf2, sems):
    fetches = []
    for c in range(8):
        part = pl.ds(c * 1024, 1024)
        fetches.append(pltpu.make_async_copy(rho.at[:, :, part], x.at[:, :, part], sems.at[0, c]))
        fetches[-1].start()
    make_plan_0(perm, T)
    for c, fetch in enumerate(fetches):
        fetch.wait()
        for k in range(8):
            lanes = slice(c * 1024 + k * 128, c * 1024 + k * 128 + 128)
            block = jnp.concatenate([x[0, :, lanes], x[1, :, lanes]], axis=0)
            buf[c * 1024 + k * 128 : c * 1024 + k * 128 + 128, :] = block.T
    sends = []
    for c in range(4):
        table_swaps(T, S0, buf, buf2, 8 * c, 8 * c + 8)
        rows = pl.ds(c * 2048, 2048)
        sends.append(pltpu.make_async_copy(buf2.at[rows], out.at[rows], sems.at[1, c]))
        sends[-1].start()
    for send in sends:
        send.wait()


def prepare_kernel(first_table, sup, T, matrices):
    def copy(k, carry):
        T[k] = first_table[k]
        return carry

    lax.fori_loop(0, TMP, copy, 0)
    make_plan_1(T)
    make_plan_2(T)
    for k, (base, out_base) in enumerate(((G, G), (G + 20, G + 20), (G + 40, G + 40), (G + 60, G + 69))):
        build_matrix(T, base, out_base, sup[k // 2], matrices.at[2 * k], matrices.at[2 * k + 1])


def mix_pass(src, dst, matrices, step, store=None):
    def body(g, carry):
        first = g * 4 if step == 1 else g
        rows = [pl.ds(pl.multiple_of((first + step * j) * 512, 512), 512) for j in range(4)]
        y = mix([src[r, :] for r in rows], matrices[0], matrices[1])
        for j in range(4):
            piece = y[:, j * 128 : (j + 1) * 128]
            if store is None:
                dst[rows[j], :] = piece
            else:
                store(g, j, piece)
        return carry

    lax.fori_loop(0, 4, body, 0)


def first_kernel(T, matrices_hbm, x, out, buf, buf2, matrices, sem, sems):
    fetch = pltpu.make_async_copy(matrices_hbm.at[pl.ds(0, 4)], matrices, sem)
    fetch.start()
    turn(x, buf2, buf, sems)
    table_swaps(T, P1, buf, buf2)
    fetch.wait()
    mix_pass(buf2, buf2, matrices.at[pl.ds(0, 2)], 1)
    strides = [T[SC + k] * 8 for k in range(10)]
    low = [jnp.int32(0)]
    for k in range(3):
        low = low + [o + strides[k] for o in low]

    def scatter(h, j, piece):
        start = jnp.bitwise_and(h, 1) * strides[6] + jnp.right_shift(h, 1) * strides[7]
        if j & 1:
            start = start + strides[8]
        if j & 2:
            start = start + strides[9]
        high = [start]
        for k in range(3, 6):
            high = high + [o + strides[k] for o in high]
        for n in range(64):
            out[tile_rows(high[n >> 3] + low[n & 7]), :] = piece[n * 8 : n * 8 + 8, :]

    mix_pass(buf2, None, matrices.at[pl.ds(2, 2)], 4, scatter)

    @pl.when(T[RARE] == 1)
    def _():
        stride = T[RARE + 1]
        amount = T[RARE + 2]
        sub = lax.broadcasted_iota(jnp.int32, (8, 128), 0)
        hit = jnp.bitwise_and(sub, amount)

        def pair(b, carry):
            low = jnp.bitwise_and(b, stride - 1)
            t = (b - low) * 2 + low
            a_rows, b_rows = tile_rows(t * 8), tile_rows((t + stride) * 8)
            a, c = out[a_rows, :], out[b_rows, :]
            up = pltpu.roll(c, amount, 0)
            down = pltpu.roll(a, 8 - amount, 0)
            out[a_rows, :] = jnp.where(hit == 0, a, up)
            out[b_rows, :] = jnp.where(hit == amount, c, down)
            return carry

        lax.fori_loop(0, 512, pair, 0)


def second_kernel(T, matrices_hbm, x, out, buf, buf2, matrices, sem, sems):
    fetch = pltpu.make_async_copy(matrices_hbm.at[pl.ds(4, 4)], matrices, sem)
    fetch.start()
    turn(x, buf2, buf, sems)
    table_swaps(T, A2, buf, buf2)
    fetch.wait()
    mix_pass(buf2, buf, matrices.at[pl.ds(0, 2)], 1)
    mix_pass(buf, buf2, matrices.at[pl.ds(2, 2)], 4)
    slots = [8 << k for k in (6, 7, 8, 0, 1, 2, 3, 4, 5, 9)]
    sublane_swaps(slots, slots, buf2, buf, (1, 2, 4))
    tiles = buf2.reshape(16, 512, 128)
    sends = []
    for c in range(4):
        transposes(T, C2, buf, buf2, 8 * c, 8 * c + 8)
        part = pl.ds(c * 128, 128)
        sends.append(pltpu.make_async_copy(tiles.at[:, part], out.at[:, part], sems.at[0, c]))
        sends[-1].start()
    for send in sends:
        send.wait()


def trace_kernel(T, pos, sup, x, out):
    step = pl.program_id(0)
    lane = lax.broadcasted_iota(jnp.int32, (8, 128), 1)
    sub = lax.broadcasted_iota(jnp.int32, (8, 128), 0)

    def bit_at(index, k, place):
        return jnp.left_shift(jnp.bitwise_and(jnp.right_shift(index, k), 1), place)

    col_base = jnp.int32(0)
    for k in range(7):
        col_base = col_base + bit_at(pos[0], k, T[WINV + T[OCCT + k]])
    col = jnp.zeros_like(lane) + col_base
    for k in range(6):
        col = col + bit_at(lane, k, T[WINV + T[OCCL + k]])
    row_sub = jnp.zeros_like(sub)
    for k in range(3):
        row_sub = row_sub + bit_at(sub, k, T[WINV + T[OCCR + k]])
    row_places = [T[WINV + T[OCCR + 3 + k]] for k in range(3)]
    tables = []
    for pair in range(2):
        v = jnp.bitwise_and(jnp.right_shift(col, 2 * pair), 3)
        for part in range(2):
            for a in range(4):
                value = jnp.zeros((8, 128), jnp.float32)
                for b in range(4):
                    index = 4 * a + b
                    total = sup[part, 0, index] + sup[part, 5, index]
                    total = total + sup[part, 10, index] + sup[part, 15, index]
                    value = jnp.where(v == b, total, value)
                tables.append(value)
    imag = lane >= 64
    high = jnp.right_shift(col, 4)

    def tile(n, total):
        g = step * 64 + n
        row = jnp.right_shift(g, 3) * 64
        for k in range(3):
            row = row + bit_at(g, k, row_places[k])
        row = row_sub + row
        factors = []
        for pair in range(2):
            u = jnp.bitwise_and(jnp.right_shift(row, 2 * pair), 3)
            for part in range(2):
                value = tables[8 * pair + 4 * part]
                for a in range(1, 4):
                    value = jnp.where(u == a, tables[8 * pair + 4 * part + a], value)
                factors.append(value)
        r0, i0, r1, i1 = factors
        weight = jnp.where(imag, -(r0 * i1 + i0 * r1), r0 * r1 - i0 * i1)
        data = x[tile_rows(n * 8), :]
        return total + jnp.where(jnp.right_shift(row, 4) == high, weight * data, 0.0)

    total = lax.fori_loop(0, 64, tile, jnp.zeros((8, 128), jnp.float32), unroll=4)

    @pl.when(step == 0)
    def _():
        out[0, 0] = jnp.float32(0.0)

    out[0, 0] = out[0, 0] + jnp.sum(total)


SMEM = pl.BlockSpec(memory_space=pltpu.SMEM)
VMEM = pl.BlockSpec(memory_space=pltpu.VMEM)
HBM = pl.BlockSpec(memory_space=pl.ANY)
LIMIT = 60 << 20
BUFFER = pltpu.VMEM((8192, 128), jnp.float32)
MATRICES = pltpu.VMEM((4, 512, 512), jnp.bfloat16)
SCRATCH = [BUFFER, BUFFER, MATRICES, pltpu.SemaphoreType.DMA, pltpu.SemaphoreType.DMA((2, 16))]


def exchange(blocks):
    return lax.all_to_all(blocks, AX, split_axis=0, concat_axis=0, tiled=True)


def per_device(rho, perm, superop):
    blocks, table = pl.pallas_call(
        split_kernel,
        in_specs=[SMEM, HBM],
        out_specs=[HBM, SMEM],
        scratch_shapes=[pltpu.VMEM((2, 64, 8192), jnp.float32), BUFFER, BUFFER, pltpu.SemaphoreType.DMA((2, 8))],
        out_shape=[
            jax.ShapeDtypeStruct((8192, 128), jnp.float32),
            jax.ShapeDtypeStruct((SIZE,), jnp.int32),
        ],
        compiler_params=pltpu.CompilerParams(vmem_limit_bytes=LIMIT),
        name="split",
    )(perm, rho)
    table, matrices = pl.pallas_call(
        prepare_kernel,
        in_specs=[SMEM, VMEM],
        out_specs=[SMEM, VMEM],
        out_shape=[
            jax.ShapeDtypeStruct((SIZE,), jnp.int32),
            jax.ShapeDtypeStruct((8, 512, 512), jnp.bfloat16),
        ],
        compiler_params=pltpu.CompilerParams(vmem_limit_bytes=LIMIT),
        name="prepare",
    )(table, superop)
    blocks = exchange(blocks.reshape(128, 64, 128))
    blocks = pl.pallas_call(
        first_kernel,
        in_specs=[SMEM, HBM, HBM],
        out_specs=VMEM,
        out_shape=jax.ShapeDtypeStruct((8192, 128), jnp.float32),
        scratch_shapes=SCRATCH,
        compiler_params=pltpu.CompilerParams(vmem_limit_bytes=LIMIT),
        name="first",
    )(table, matrices, blocks.reshape(8192, 128))
    device = lax.axis_index(AX).astype(jnp.int32).reshape(1)
    trace = pl.pallas_call(
        trace_kernel,
        grid=(16,),
        in_specs=[SMEM, SMEM, SMEM, pl.BlockSpec((512, 128), lambda i: (i, 0))],
        out_specs=SMEM,
        out_shape=jax.ShapeDtypeStruct((1, 1), jnp.float32),
        name="trace",
    )(table, device, superop[1], blocks)
    blocks = exchange(blocks.reshape(128, 64, 128))
    blocks, trace = lax.optimization_barrier((blocks, trace))
    parts = exchange(jnp.broadcast_to(trace[0, 0], (128, 1, 128)))
    tiles = pl.pallas_call(
        second_kernel,
        in_specs=[SMEM, HBM, HBM],
        out_specs=HBM,
        out_shape=jax.ShapeDtypeStruct((16, 512, 128), jnp.float32),
        scratch_shapes=SCRATCH,
        compiler_params=pltpu.CompilerParams(vmem_limit_bytes=LIMIT),
        name="second",
    )(table, matrices, blocks.reshape(8192, 128))
    rho_out = tiles.reshape(2, 8, 64, 8, 128).transpose(0, 1, 3, 2, 4).reshape(2, 64, 8192)
    return rho_out, jnp.sum(parts[:, 0, 0]) / ROWS


def solution(mesh):
    spec = P(None, AX, None)
    return jax.shard_map(
        per_device, mesh=mesh, in_specs=(spec, P(), P()), out_specs=(spec, P()), check_vma=False
    )
```

```python
import jax
import jax.numpy as jnp
from jax import lax
from jax.experimental import pallas as pl
from jax.experimental.pallas import tpu as pltpu
from jax.sharding import PartitionSpec as P

ROWS = 8192
AX = ("hi", "grp")
RI = 13

W = 0
WINV = 16
U = 32
S0 = 48
A2 = 80
C2 = 112
P1 = 176
SC = 208
RARE = 220
G = 224
OCCL = 320
OCCT = 328
OCCR = 336
SUBC = 344
TMP = 352
OCC = 384
USED = 400
SIZE = 432


def pick(cond, a, b):
    return jnp.where(cond, jnp.int32(a), jnp.int32(b))


def lane_of(T, lanes, x):
    lane = jnp.int32(0)
    for p in range(7):
        lane = pick(T[lanes + p] == x, p, lane)
    return lane


def other_lanes(T, base, taken):
    for p in range(7):
        T[TMP + p] = jnp.int32(0)
    for lane in taken:
        T[TMP + lane] = jnp.int32(1)
    for k in range(4):
        free = jnp.int32(0)
        for p in range(7):
            free = pick(T[TMP + p] == 0, p, free)
        T[TMP + free] = jnp.int32(1)
        T[base + 5 + k] = free


def fill_slots(T, base, done, slots=10):
    for k in range(slots):
        free = jnp.int32(0)
        for s in range(slots):
            free = pick(T[USED + s] == 0, s, free)
        if k < done:
            free = jnp.where(T[base + k] >= 0, T[base + k], free)
        T[USED + free] = jnp.int32(1)
        T[base + k] = free


def set_strides(T, base, target):
    for k in range(10):
        s = T[base + k]
        T[base + k] = jnp.left_shift(jnp.int32(1), s)
        T[base + 10 + k] = jnp.left_shift(jnp.int32(1), T[target + s])


def make_plan_0(perm, T):
    one = jnp.int32(1)
    for q in range(13):
        w = perm[0, perm[1, q]]
        T[W + q] = w
        T[WINV + w] = jnp.int32(q)
    for b in range(16):
        T[TMP + b] = jnp.int32(0)
        T[USED + b] = jnp.int32(0)
    for q in range(4):
        T[TMP + T[W + q]] = jnp.int32(2)
    for j in range(4):
        T[U + j] = perm[0, j]
        T[TMP + perm[0, j]] = one
    for _ in range(2):
        x = jnp.int32(0)
        for b in range(12, -1, -1):
            x = pick(T[TMP + b] == 0, b, x)
        T[TMP + x] = one
    for s in range(10):
        T[OCC + s] = jnp.int32(3 + s)
    for i in range(3):
        best = jnp.int32(-1)
        for s in range(10):
            good = jnp.logical_and(T[TMP + 3 + s] == 1, T[USED + s] == 0)
            best = pick(good, s, best)
        slot = jnp.where(T[TMP + i] == 1, -1, best)
        active = slot >= 0
        safe = jnp.maximum(slot, 0)
        T[USED + safe] = jnp.where(active, one, T[USED + safe])
        T[OCCL + i] = jnp.where(active, slot + 3, jnp.int32(i))
        T[OCC + safe] = jnp.where(active, jnp.int32(i), T[OCC + safe])
        T[S0 + i] = slot
        T[S0 + 20 + i] = pick(active, 1 << i, 0)
    for k in range(10):
        free = jnp.int32(0)
        best = jnp.int32(-1)
        for s in range(10):
            unused = T[USED + s] == 0
            free = pick(unused, s, free)
            best = pick(jnp.logical_and(unused, T[TMP + T[OCC + s]] == 1), s, best)
        free = jnp.where(best >= 0, best, free)
        if k < 3:
            free = jnp.where(T[S0 + k] >= 0, T[S0 + k], free)
        T[USED + free] = one
        T[S0 + k] = free
    kept = jnp.int32(0)
    sent = jnp.int32(0)
    for k in range(10):
        s = T[S0 + k]
        occ = T[OCC + s]
        is_kept = T[TMP + occ] == 1
        T[USED + s] = jnp.where(is_kept, kept, sent + 3)
        T[jnp.where(is_kept, OCCL + 3 + kept, OCCT + sent)] = occ
        kept = jnp.where(is_kept, kept + 1, kept)
        sent = jnp.where(is_kept, sent, sent + 1)
    T[OCCL + 6] = jnp.int32(RI)
    set_strides(T, S0, USED)


def make_plan_1(T):
    one = jnp.int32(1)
    u = tuple(T[U + j] for j in range(4))
    for k in range(2):
        base = G + 20 * k
        lanes = [lane_of(T, OCCL, x) for x in (RI, u[2 * k], u[2 * k + 1])]
        other_lanes(T, base, lanes)
        for p in range(3):
            T[base + p] = lanes[p]
        T[base + 3] = jnp.int32(7)
        T[base + 4] = jnp.int32(8)
    for b in range(16):
        T[TMP + b] = jnp.int32(0)
        T[USED + b] = jnp.int32(0)
    for j in range(4):
        T[TMP + u[j]] = one
    for s in range(10):
        T[OCC + s] = jnp.int32(3 + s)
    for i in range(3):
        mine_u = T[TMP + i]
        mine_ok = jnp.logical_and(mine_u == 0, T[WINV + i] < 6)
        best = jnp.int32(-1)
        spare = jnp.int32(-1)
        for b in range(3, 13):
            free = jnp.logical_and(T[TMP + b] == 0, T[USED + b - 3] == 0)
            spare = pick(free, b, spare)
            best = pick(jnp.logical_and(free, T[WINV + b] < 6), b, best)
        other = jnp.where(mine_u == 0, -1, spare)
        bit = jnp.where(mine_ok, -1, jnp.where(best >= 0, best, other))
        active = bit >= 0
        safe = jnp.maximum(bit, 3)
        T[USED + safe - 3] = jnp.where(active, one, T[USED + safe - 3])
        T[P1 + i] = jnp.where(active, bit - 3, -1)
        T[OCCR + i] = jnp.where(active, bit, jnp.int32(i))
        T[OCC + safe - 3] = jnp.where(active, jnp.int32(i), T[OCC + safe - 3])
        T[P1 + 20 + i] = pick(active, 1 << i, 0)
    fill_slots(T, P1, 3)
    rare = jnp.int32(0)
    rare_amt = jnp.int32(0)
    rare_q = jnp.int32(6)
    for i in range(3):
        q = T[WINV + T[OCCR + i]]
        bad = q >= 6
        rare = pick(bad, 1, rare)
        rare_amt = pick(bad, 1 << i, rare_amt)
        rare_q = jnp.where(bad, q, rare_q)
    other = jnp.int32(0)
    kept = jnp.int32(0)
    rare_bit = jnp.int32(0)
    for s in range(10):
        occ = T[OCC + s]
        in_u = jnp.int32(-1)
        for j in range(4):
            in_u = pick(occ == u[j], 6 + j, in_u)
        place = jnp.where(in_u >= 0, in_u, other)
        other = jnp.where(in_u >= 0, other, other + 1)
        T[TMP + s] = place
        q = T[WINV + occ]
        is_kept = q < 6
        fits = kept < 3
        bit = jnp.where(is_kept, jnp.where(fits, kept, rare_q - 3), q - 3)
        slot = jnp.where(jnp.logical_and(is_kept, fits), kept, 3)
        T[OCCR + 3 + slot] = jnp.where(is_kept, occ, jnp.int32(RI))
        rare_bit = jnp.where(jnp.logical_and(is_kept, jnp.logical_not(fits)), occ, rare_bit)
        kept = jnp.where(is_kept, kept + 1, kept)
        T[SC + place] = jnp.left_shift(one, bit)
    for i in range(3):
        q = T[WINV + T[OCCR + i]]
        T[OCCR + i] = jnp.where(q >= 6, rare_bit, T[OCCR + i])
    T[OCCR + 6] = jnp.int32(RI)
    T[RARE] = rare
    T[RARE + 1] = jnp.left_shift(one, rare_q - 3)
    T[RARE + 2] = rare_amt
    set_strides(T, P1, TMP)


def make_plan_2(T):
    one = jnp.int32(1)
    w = tuple(T[W + q] for q in range(13))
    for k in range(3):
        T[SUBC + k] = T[OCCL + k]
        T[OCC + k] = T[OCCL + 3 + k]
    for k in range(7):
        T[OCC + 3 + k] = T[OCCT + k]
    for s in range(16):
        T[USED + s] = jnp.int32(0)
    for i in range(3):
        mine = T[SUBC + i]
        best = jnp.int32(-1)
        for s in range(10):
            good = jnp.logical_and(T[WINV + T[OCC + s]] >= 4, T[USED + s] == 0)
            best = pick(good, s, best)
        slot = jnp.where(T[WINV + mine] >= 4, -1, best)
        active = slot >= 0
        safe = jnp.maximum(slot, 0)
        T[USED + safe] = jnp.where(active, one, T[USED + safe])
        new = T[OCC + safe]
        T[SUBC + i] = jnp.where(active, new, mine)
        T[OCC + safe] = jnp.where(active, mine, new)
        T[A2 + i] = slot
        T[A2 + 20 + i] = pick(active, 1 << i, 0)
    fill_slots(T, A2, 3)
    other = jnp.int32(0)
    for s in range(10):
        q = T[WINV + T[OCC + s]]
        T[TMP + s] = jnp.where(q < 4, q + 6, other)
        other = jnp.where(q < 4, other, other + 1)
    set_strides(T, A2, TMP)
    for s in range(10):
        T[USED + T[TMP + s]] = T[OCC + s]
    for s in range(10):
        T[OCC + s] = T[USED + s]
    rows = [lane_of(T, OCCR, w[q]) for q in range(6)]
    ri = lane_of(T, OCCR, RI)
    other_lanes(T, G + 40, (ri, rows[0], rows[1]))
    for k, v in enumerate((ri, 7, 8, rows[0], rows[1])):
        T[G + 40 + k] = jnp.int32(v)
    for k, v in enumerate((ri, 7, 8, rows[2], rows[3], rows[0], rows[1], rows[4], rows[5])):
        T[G + 60 + k] = jnp.int32(v)
    for k, v in enumerate((6, 7, 8, 2, 3, 0, 1, 4, 5)):
        T[G + 69 + k] = jnp.int32(v)
    for i in range(3):
        T[OCC + 6 + i] = T[SUBC + i]
    for s in range(10):
        T[TMP + s] = T[WINV + T[OCC + s]] - 7
    for k in range(10):
        slot = jnp.int32(0)
        for s in range(10):
            slot = pick(T[OCC + s] == w[3 + k], s, slot)
        T[C2 + k] = slot
        if k < 4:
            T[TMP + slot] = jnp.int32(6 + k)
    set_strides(T, C2, TMP)


def sums(start, strides):
    out = [start]
    for stride in strides:
        out = out + [o + stride for o in out]
    return out


def block_loop(src, dst, load, store, work, first=0, last=32):
    src_low = sums(jnp.int32(0), src[:3])
    dst_low = sums(jnp.int32(0), dst[:3])

    def block(b, carry):
        src_base = jnp.int32(0)
        dst_base = jnp.int32(0)
        for k in range(5):
            bit = jnp.bitwise_and(jnp.right_shift(b, k), 1)
            src_base = src_base + bit * src[5 + k]
            dst_base = dst_base + bit * dst[5 + k]
        vs = []
        for high in sums(src_base, src[3:5]):
            vs.extend(load[tile_rows(high + low), :] for low in src_low)
        vs = work(vs)
        m = 0
        for high in sums(dst_base, dst[3:5]):
            for low in dst_low:
                store[tile_rows(high + low), :] = vs[m]
                m += 1
        return carry

    lax.fori_loop(first, last, block, 0)


def table_strides(T, base):
    return [T[base + k] * 8 for k in range(10)], [T[base + 10 + k] * 8 for k in range(10)]


def sublane_swaps(src, dst, load, store, amounts, first=0, last=32):
    sub = lax.broadcasted_iota(jnp.int32, (8, 128), 0)
    hits = [jnp.bitwise_and(sub, amount) for amount in amounts]
    keep_x = [hit == 0 for hit in hits]
    keep_y = [hit == amount for hit, amount in zip(hits, amounts)]

    def work(vs):
        for k in range(3):
            for m in range(32):
                if not m >> k & 1:
                    n = m | 1 << k
                    x, y = vs[m], vs[n]
                    vs[m] = jnp.where(keep_x[k], x, pltpu.roll(y, 1 << k, 0))
                    vs[n] = jnp.where(keep_y[k], y, pltpu.roll(x, 8 - (1 << k), 0))
        return vs

    block_loop(src, dst, load, store, work, first, last)


def table_swaps(T, base, load, store, first=0, last=32):
    src, dst = table_strides(T, base)
    sublane_swaps(src, dst, load, store, [T[base + 20 + k] for k in range(3)], first, last)


def transposes(T, base, load, store, first, last):
    src, dst = table_strides(T, base)

    def work(vs):
        out = []
        for half in range(2):
            y = jnp.concatenate(vs[16 * half : 16 * half + 16], axis=0).T
            out.extend(y[8 * m : 8 * m + 8, :] for m in range(16))
        return out

    block_loop(src, dst, load, store, work, first, last)


def turn(hbm, src, dst, sems):
    low = lax.broadcasted_iota(jnp.int32, (64, 128), 1) < 64

    def copies(c):
        out = []
        for half in range(2):
            rows = pl.ds(pl.multiple_of(half * 4096 + c * 256, 256), 256)
            out.append(pltpu.make_async_copy(hbm.at[rows], src.at[rows], sems.at[half, c]))
        return out

    for c in range(16):
        for copy in copies(c):
            copy.start()

    def body(c, carry):
        for copy in copies(c):
            copy.wait()
        for k in range(4):
            rows = [pl.ds(pl.multiple_of(half * 4096 + c * 256 + k * 64, 64), 64) for half in range(2)]
            y = jnp.concatenate([src[r, :] for r in rows], axis=0).T
            p, q = y[:64, :], y[64:, :]
            moved = pltpu.roll(jnp.where(low, q, p), 64, 1)
            dst[rows[0], :] = jnp.where(low, p, moved)
            dst[rows[1], :] = jnp.where(low, moved, q)
        return carry

    lax.fori_loop(0, 16, body, 0)


def tile_rows(row):
    return pl.ds(pl.multiple_of(row, 8), 8)


def build_matrix(T, base, out_base, sup, gh_ref, gl_ref):
    real, imag = sup[0], sup[1]
    top = jnp.concatenate([real, -imag], axis=1)
    bottom = jnp.concatenate([imag, real], axis=1)
    kern = jnp.concatenate([top, bottom], axis=0)
    index_i = lax.broadcasted_iota(jnp.int32, (512, 32), 0)
    index_o = lax.broadcasted_iota(jnp.int32, (32, 512), 1)

    def code(index, start, first, count):
        total = jnp.zeros_like(index)
        place = {0: 4, 1: 0, 2: 1, 3: 2, 4: 3}
        for k in range(first, first + count):
            bit = jnp.bitwise_and(jnp.right_shift(index, T[start + k]), 1)
            total = total + jnp.left_shift(bit, place[k] if first == 0 else k - first)
        return total

    one_i = (code(index_i, base, 0, 5) == lax.broadcasted_iota(jnp.int32, (512, 32), 1)).astype(jnp.bfloat16)
    one_o = (code(index_o, out_base, 0, 5) == lax.broadcasted_iota(jnp.int32, (32, 512), 0)).astype(jnp.bfloat16)
    rest_i = code(lax.broadcasted_iota(jnp.int32, (512, 128), 0), base, 5, 4)
    rest_o = code(lax.broadcasted_iota(jnp.int32, (8, 512), 1), out_base, 5, 4)
    same = jnp.concatenate([rest_i] * 4, axis=1) == jnp.concatenate([rest_o] * 64, axis=0)
    kh = kern.astype(jnp.bfloat16)
    kl = (kern - kh.astype(jnp.float32)).astype(jnp.bfloat16)
    for part, ref in ((kh, gh_ref), (kl, gl_ref)):
        left = lax.dot_general(one_i, part, (((1,), (1,)), ((), ())), preferred_element_type=jnp.float32)
        full = jnp.dot(left.astype(jnp.bfloat16), one_o, preferred_element_type=jnp.float32)
        ref[...] = jnp.where(same, full, 0.0).astype(jnp.bfloat16)


def mix(parts, gh, gl):
    x = jnp.concatenate(parts, axis=1)
    xh = x.astype(jnp.bfloat16)
    xl = (x - xh.astype(jnp.float32)).astype(jnp.bfloat16)
    y = jnp.dot(xl, gh, preferred_element_type=jnp.float32)
    y = y + jnp.dot(xh, gl, preferred_element_type=jnp.float32)
    return y + jnp.dot(xh, gh, preferred_element_type=jnp.float32)


def split_kernel(perm, rho, out, T, x, buf, buf2, sems):
    fetches = []
    for c in range(8):
        part = pl.ds(c * 1024, 1024)
        fetches.append(pltpu.make_async_copy(rho.at[:, :, part], x.at[:, :, part], sems.at[0, c]))
        fetches[-1].start()
    make_plan_0(perm, T)
    for c, fetch in enumerate(fetches):
        fetch.wait()
        for k in range(8):
            lanes = slice(c * 1024 + k * 128, c * 1024 + k * 128 + 128)
            block = jnp.concatenate([x[0, :, lanes], x[1, :, lanes]], axis=0)
            buf[c * 1024 + k * 128 : c * 1024 + k * 128 + 128, :] = block.T
    sends = []
    for c in range(4):
        table_swaps(T, S0, buf, buf2, 8 * c, 8 * c + 8)
        rows = pl.ds(c * 2048, 2048)
        sends.append(pltpu.make_async_copy(buf2.at[rows], out.at[rows], sems.at[1, c]))
        sends[-1].start()
    for send in sends:
        send.wait()


def prepare_kernel(first_table, sup, T, matrices):
    def copy(k, carry):
        T[k] = first_table[k]
        return carry

    lax.fori_loop(0, TMP, copy, 0)
    make_plan_1(T)
    make_plan_2(T)
    for k, (base, out_base) in enumerate(((G, G), (G + 20, G + 20), (G + 40, G + 40), (G + 60, G + 69))):
        build_matrix(T, base, out_base, sup[k // 2], matrices.at[2 * k], matrices.at[2 * k + 1])


def mix_pass(src, dst, matrices, step, store=None):
    def body(g, carry):
        first = g * 4 if step == 1 else g
        rows = [pl.ds(pl.multiple_of((first + step * j) * 512, 512), 512) for j in range(4)]
        y = mix([src[r, :] for r in rows], matrices[0], matrices[1])
        for j in range(4):
            piece = y[:, j * 128 : (j + 1) * 128]
            if store is None:
                dst[rows[j], :] = piece
            else:
                store(g, j, piece)
        return carry

    lax.fori_loop(0, 4, body, 0)


def first_kernel(T, matrices_hbm, x, out, buf, buf2, matrices, sem, sems):
    fetch = pltpu.make_async_copy(matrices_hbm.at[pl.ds(0, 4)], matrices, sem)
    fetch.start()
    turn(x, buf2, buf, sems)
    table_swaps(T, P1, buf, buf2)
    fetch.wait()
    mix_pass(buf2, buf2, matrices.at[pl.ds(0, 2)], 1)
    strides = [T[SC + k] * 8 for k in range(10)]
    low = [jnp.int32(0)]
    for k in range(3):
        low = low + [o + strides[k] for o in low]

    def scatter(h, j, piece):
        start = jnp.bitwise_and(h, 1) * strides[6] + jnp.right_shift(h, 1) * strides[7]
        if j & 1:
            start = start + strides[8]
        if j & 2:
            start = start + strides[9]
        high = [start]
        for k in range(3, 6):
            high = high + [o + strides[k] for o in high]
        for n in range(64):
            out[tile_rows(high[n >> 3] + low[n & 7]), :] = piece[n * 8 : n * 8 + 8, :]

    mix_pass(buf2, None, matrices.at[pl.ds(2, 2)], 4, scatter)

    @pl.when(T[RARE] == 1)
    def _():
        stride = T[RARE + 1]
        amount = T[RARE + 2]
        sub = lax.broadcasted_iota(jnp.int32, (8, 128), 0)
        hit = jnp.bitwise_and(sub, amount)

        def pair(b, carry):
            low = jnp.bitwise_and(b, stride - 1)
            t = (b - low) * 2 + low
            a_rows, b_rows = tile_rows(t * 8), tile_rows((t + stride) * 8)
            a, c = out[a_rows, :], out[b_rows, :]
            up = pltpu.roll(c, amount, 0)
            down = pltpu.roll(a, 8 - amount, 0)
            out[a_rows, :] = jnp.where(hit == 0, a, up)
            out[b_rows, :] = jnp.where(hit == amount, c, down)
            return carry

        lax.fori_loop(0, 512, pair, 0)


def second_kernel(T, matrices_hbm, x, out, buf, buf2, matrices, sem, sems):
    fetch = pltpu.make_async_copy(matrices_hbm.at[pl.ds(4, 4)], matrices, sem)
    fetch.start()
    turn(x, buf2, buf, sems)
    table_swaps(T, A2, buf, buf2)
    fetch.wait()
    mix_pass(buf2, buf, matrices.at[pl.ds(0, 2)], 1)
    mix_pass(buf, buf2, matrices.at[pl.ds(2, 2)], 4)
    slots = [8 << k for k in (6, 7, 8, 0, 1, 2, 3, 4, 5, 9)]
    sublane_swaps(slots, slots, buf2, buf, (1, 2, 4))
    tiles = buf2.reshape(16, 512, 128)
    sends = []
    for c in range(4):
        transposes(T, C2, buf, buf2, 8 * c, 8 * c + 8)
        part = pl.ds(c * 128, 128)
        sends.append(pltpu.make_async_copy(tiles.at[:, part], out.at[:, part], sems.at[0, c]))
        sends[-1].start()
    for send in sends:
        send.wait()


def trace_kernel(T, pos, sup, x, out, acc):
    step = pl.program_id(0)
    lane = lax.broadcasted_iota(jnp.int32, (8, 128), 1)
    sub = lax.broadcasted_iota(jnp.int32, (8, 128), 0)

    def bit_at(index, k, place):
        return jnp.left_shift(jnp.bitwise_and(jnp.right_shift(index, k), 1), place)

    col_base = jnp.int32(0)
    for k in range(7):
        col_base = col_base + bit_at(pos[0], k, T[WINV + T[OCCT + k]])
    col = jnp.zeros_like(lane) + col_base
    for k in range(6):
        col = col + bit_at(lane, k, T[WINV + T[OCCL + k]])
    row_sub = jnp.zeros_like(sub)
    for k in range(3):
        row_sub = row_sub + bit_at(sub, k, T[WINV + T[OCCR + k]])
    row_places = [T[WINV + T[OCCR + 3 + k]] for k in range(3)]
    tables = []
    for pair in range(2):
        v = jnp.bitwise_and(jnp.right_shift(col, 2 * pair), 3)
        for part in range(2):
            for a in range(4):
                value = jnp.zeros((8, 128), jnp.float32)
                for b in range(4):
                    index = 4 * a + b
                    total = sup[part, 0, index] + sup[part, 5, index]
                    total = total + sup[part, 10, index] + sup[part, 15, index]
                    value = jnp.where(v == b, total, value)
                tables.append(value)
    imag = lane >= 64
    high = jnp.right_shift(col, 4)

    def tile(n, total):
        g = step * 64 + n
        row = jnp.right_shift(g, 3) * 64
        for k in range(3):
            row = row + bit_at(g, k, row_places[k])
        row = row_sub + row
        factors = []
        for pair in range(2):
            u = jnp.bitwise_and(jnp.right_shift(row, 2 * pair), 3)
            for part in range(2):
                value = tables[8 * pair + 4 * part]
                for a in range(1, 4):
                    value = jnp.where(u == a, tables[8 * pair + 4 * part + a], value)
                factors.append(value)
        r0, i0, r1, i1 = factors
        weight = jnp.where(imag, -(r0 * i1 + i0 * r1), r0 * r1 - i0 * i1)
        data = x[tile_rows(n * 8), :]
        return total + jnp.where(jnp.right_shift(row, 4) == high, weight * data, 0.0)

    total = lax.fori_loop(0, 64, tile, jnp.zeros((8, 128), jnp.float32), unroll=4)

    @pl.when(step == 0)
    def _():
        acc[0] = jnp.float32(0.0)

    acc[0] = acc[0] + jnp.sum(total)

    @pl.when(step == 15)
    def _():
        out[...] = jnp.full((128, 1, 128), acc[0], jnp.float32)


SMEM = pl.BlockSpec(memory_space=pltpu.SMEM)
VMEM = pl.BlockSpec(memory_space=pltpu.VMEM)
HBM = pl.BlockSpec(memory_space=pl.ANY)
LIMIT = 60 << 20
BUFFER = pltpu.VMEM((8192, 128), jnp.float32)
MATRICES = pltpu.VMEM((4, 512, 512), jnp.bfloat16)
SCRATCH = [BUFFER, BUFFER, MATRICES, pltpu.SemaphoreType.DMA, pltpu.SemaphoreType.DMA((2, 16))]


def exchange(blocks):
    return lax.all_to_all(blocks, AX, split_axis=0, concat_axis=0, tiled=True)


def per_device(rho, perm, superop):
    blocks, table = pl.pallas_call(
        split_kernel,
        in_specs=[SMEM, HBM],
        out_specs=[HBM, SMEM],
        scratch_shapes=[pltpu.VMEM((2, 64, 8192), jnp.float32), BUFFER, BUFFER, pltpu.SemaphoreType.DMA((2, 8))],
        out_shape=[
            jax.ShapeDtypeStruct((8192, 128), jnp.float32),
            jax.ShapeDtypeStruct((SIZE,), jnp.int32),
        ],
        compiler_params=pltpu.CompilerParams(vmem_limit_bytes=LIMIT),
        name="split",
    )(perm, rho)
    table, matrices = pl.pallas_call(
        prepare_kernel,
        in_specs=[SMEM, VMEM],
        out_specs=[SMEM, VMEM],
        out_shape=[
            jax.ShapeDtypeStruct((SIZE,), jnp.int32),
            jax.ShapeDtypeStruct((8, 512, 512), jnp.bfloat16),
        ],
        compiler_params=pltpu.CompilerParams(vmem_limit_bytes=LIMIT),
        name="prepare",
    )(table, superop)
    blocks = exchange(blocks.reshape(128, 64, 128))
    blocks = pl.pallas_call(
        first_kernel,
        in_specs=[SMEM, HBM, HBM],
        out_specs=VMEM,
        out_shape=jax.ShapeDtypeStruct((8192, 128), jnp.float32),
        scratch_shapes=SCRATCH,
        compiler_params=pltpu.CompilerParams(vmem_limit_bytes=LIMIT),
        name="first",
    )(table, matrices, blocks.reshape(8192, 128))
    device = lax.axis_index(AX).astype(jnp.int32).reshape(1)
    trace = pl.pallas_call(
        trace_kernel,
        grid=(16,),
        in_specs=[SMEM, SMEM, SMEM, pl.BlockSpec((512, 128), lambda i: (i, 0))],
        out_specs=pl.BlockSpec((128, 1, 128), lambda i: (0, 0, 0)),
        out_shape=jax.ShapeDtypeStruct((128, 1, 128), jnp.float32),
        scratch_shapes=[pltpu.SMEM((1,), jnp.float32)],
        name="trace",
    )(table, device, superop[1], blocks)
    blocks = exchange(blocks.reshape(128, 64, 128))
    blocks, trace = lax.optimization_barrier((blocks, trace))
    parts = exchange(trace)
    tiles = pl.pallas_call(
        second_kernel,
        in_specs=[SMEM, HBM, HBM],
        out_specs=HBM,
        out_shape=jax.ShapeDtypeStruct((16, 512, 128), jnp.float32),
        scratch_shapes=SCRATCH,
        compiler_params=pltpu.CompilerParams(vmem_limit_bytes=LIMIT),
        name="second",
    )(table, matrices, blocks.reshape(8192, 128))
    rho_out = tiles.reshape(2, 8, 64, 8, 128).transpose(0, 1, 3, 2, 4).reshape(2, 64, 8192)
    return rho_out, jnp.sum(parts[:, 0, 0]) / ROWS


def solution(mesh):
    spec = P(None, AX, None)
    return jax.shard_map(
        per_device, mesh=mesh, in_specs=(spec, P(), P()), out_specs=(spec, P()), check_vma=False
    )
```
